32 devices in a mesh: gx: 4 (over y, core), gy: 2 (over x), gz: 4 (over z).
Axes of the slice: x: 2, y: 2, z: 4, core: 2. Of those that a mesh axis runs over, the one named last changes fastest.
Arguments:
- offsets: float32 [3, 110592], P(None, ('gx', 'gy', 'gz')), may hold values from 0 to 1
- velocities: float32 [3, 110592], P(None, ('gx', 'gy', 'gz')), may hold values from -6 to 6
- masses: float32 [110592], P(('gx', 'gy', 'gz')), may hold values from 0.5 to 2
- active: int32 [110592], P(('gx', 'gy', 'gz')), may hold values from 0 to 1, as said below
- near_local: int32 [864, 2], P(('gx', 'gy', 'gz')), may hold values from 0 to 26
- near_remote: int32 [864, 3, 1], P(('gx', 'gy', 'gz')), may hold values from 0 to 8
- far_list: int32 [864, 5, 2], P(('gx', 'gy', 'gz')), may hold values from 0 to 26
Outputs:
- positions_out: float32 [3, 110592], P(None, ('gx', 'gy', 'gz'))
- velocities_out: float32 [3, 110592], P(None, ('gx', 'gy', 'gz'))
- accel_out: float32 [3, 110592], P(None, ('gx', 'gy', 'gz'))
- time_steps: float32 [2], replicated
The draws below stay inside these ranges and needn't reach their ends.
Inputs may be any that keep to these rules, and one draw needn't show every extreme that they name: `active`: 0 or 1; each device has its own rate of ones, from 1/64 to 1/4.
All inputs are finite; a program needn't handle non-finite values.
Results may differ from the reference program's by a relative error of at most 0.0003.
Values sent between devices are 32-bit elements; how exact they have to be, the bound alone decides.
No kernel may reach another device: no remote copies, remote signals or barrier semaphores. Data moves between devices by JAX's collectives and lax.ppermute only.
A program may use at most 64 MiB of HBM per device.

```python
import math
import jax
import jax.numpy as jnp
from jax import lax

TILE = 128
TG = 3
KL = 2
KN = 1
KM = 2
SUBSTEPS = 2
NT = 27
NB = 9
LEVELS = 5
NTILES = 864
NPART = 110592
N_GY = 2
N_GZ = 4


def draw_active(key, part):
    rate_key = jax.random.fold_in(key, 11)
    ticket_key = jax.random.fold_in(key, 12)
    devices = NPART // (NT * TILE)
    rates = jax.random.randint(rate_key, (devices, 1), 1, 17)
    tickets = jax.random.randint(ticket_key, (devices, NT * TILE), 0, 64)
    return (tickets < rates).astype(jnp.int32).reshape(NPART)


def with_ends(values, own_key, low, high):
    longest = values.shape.index(max(values.shape))
    spots = []
    for shift in (0, 1):
        where = [jax.random.randint(jax.random.fold_in(own_key, axis), (), 0, length) for axis, length in enumerate(values.shape)]
        where[longest] = (where[longest] + shift) % values.shape[longest]
        spots.append(tuple(where))
    return values.at[spots[0]].set(low).at[spots[1]].set(high)


def steps_of(key, shape, split, low, top_value):
    loudness = 1.0
    for dim, blocks in split:
        draws = jax.random.uniform(jax.random.fold_in(jax.random.fold_in(key, 6), dim), (blocks,), jnp.float32, low / len(split), top_value / len(split))
        loudness = loudness * jnp.repeat(jnp.exp(draws), shape[dim] // blocks).reshape((-1,) + (1,) * (len(shape) - 1 - dim))
    return loudness


def centred(stream_key, shape, width, most, cuts=(), kind=jnp.bfloat16):
    gain = steps_of(stream_key, shape, cuts, -0.22, 0.18) if cuts else 1.0
    values = jax.random.normal(stream_key, shape, jnp.float32) * width * gain
    return jnp.minimum(jnp.maximum(values, -most), most).astype(kind)


def setup_inputs(seed: int = 0) -> dict:
    key_of = jax.random.split(jax.random.key(seed), 8)
    offsets = jnp.clip(1.0 * jax.random.uniform(key_of[0], (3, NPART), jnp.float32) ** steps_of(key_of[0], (3, NPART), ((1, 32),), -0.2, 0.2), 0.0, 1.0)
    velocities = centred(key_of[1], (3, NPART), 1.0, 6.0, ((1, 32),), jnp.float32)
    masses = jnp.clip(jnp.exp(math.log(2.0) - 1.3862944 * jax.random.uniform(key_of[2], (NPART,), jnp.float32) ** steps_of(key_of[2], (NPART,), ((0, 32),), -0.2, 0.2)), 0.5, 2.0)
    active = draw_active(jax.random.fold_in(key_of[7], 71), 0)
    near_local = with_ends(jax.random.randint(key_of[4], (NTILES, KL), 0, NT), jax.random.fold_in(key_of[4], 1), 0, NT - 1).astype(jnp.int32)
    near_remote = with_ends(jax.random.randint(key_of[5], (NTILES, 3, KN), 0, NB), jax.random.fold_in(key_of[5], 1), 0, NB - 1).astype(jnp.int32)
    far_list = with_ends(jax.random.randint(key_of[6], (NTILES, LEVELS, KM), 0, NT), jax.random.fold_in(key_of[6], 1), 0, NT - 1).astype(jnp.int32)
    return dict(offsets=offsets, velocities=velocities, masses=masses, active=active, near_local=near_local, near_remote=near_remote, far_list=far_list)


GRAV = 0.02
SOFT2 = 0.0025
ETA = 0.15

def tile_corners(tile_grid):
    tile_ids = jnp.arange(tile_grid ** 3, dtype=jnp.int32)
    return jnp.stack([tile_ids // (tile_grid * tile_grid), tile_ids // tile_grid % tile_grid, tile_ids % tile_grid]).astype(jnp.float32)

def tile_moments(bodies):
    tile_mass = bodies[3]
    total_mass = lax.optimization_barrier(jnp.sum(tile_mass, axis=-1))
    center = lax.optimization_barrier(jnp.sum(bodies[:3] * tile_mass, axis=-1)) / total_mass
    relative = bodies[:3] - center[:, :, None]
    square = lax.optimization_barrier(jnp.sum(relative * relative, axis=0))

    def quad(first_axis, second_axis):
        quad_term = 3.0 * relative[first_axis] * relative[second_axis]
        if first_axis == second_axis:
            quad_term = quad_term - square
        return lax.optimization_barrier(jnp.sum(tile_mass * quad_term, axis=-1))
    return jnp.stack([total_mass, center[0], center[1], center[2], quad(0, 0), quad(1, 1), quad(2, 2), quad(0, 1), quad(0, 2), quad(1, 2)])

def face_index(cut_axis, face_coord, tile_grid):
    strides = (tile_grid * tile_grid, tile_grid, 1)
    others = [axis_id for axis_id in range(3) if axis_id != cut_axis]
    slot_ids = jnp.arange(tile_grid * tile_grid, dtype=jnp.int32)
    return face_coord * strides[cut_axis] + slot_ids // tile_grid * strides[others[0]] + slot_ids % tile_grid * strides[others[1]]

def level_place(level, z_bits, y_bits):
    if level < z_bits:
        return (2, level, 0 if level == 0 else -1)
    if level < z_bits + y_bits:
        return (1, level - z_bits, 1 if level == z_bits else -1)
    return (0, level - z_bits - y_bits, 2 if level == z_bits + y_bits else -1)

def signed_shift(own_bit, span):
    return jnp.where(own_bit == 0, span, -span).astype(jnp.float32)

def far_field(target, moments):
    relative = target[:, :, None] - moments[1:4, None, :]
    distance = lax.optimization_barrier(jnp.sum(relative * relative, axis=0)) + SOFT2
    inverse = lax.rsqrt(distance)
    inverse_sq = inverse * inverse
    cube = inverse * inverse_sq
    fifth = cube * inverse_sq
    seventh = fifth * inverse_sq
    quad_dot = jnp.stack([moments[4] * relative[0] + moments[7] * relative[1] + moments[8] * relative[2], moments[7] * relative[0] + moments[5] * relative[1] + moments[9] * relative[2], moments[8] * relative[0] + moments[9] * relative[1] + moments[6] * relative[2]])
    quad_form = lax.optimization_barrier(jnp.sum(relative * quad_dot, axis=0))
    field = -moments[0] * relative * cube + quad_dot * fifth - 2.5 * quad_form * relative * seventh
    return lax.optimization_barrier(jnp.sum(field, axis=2))

def tile_force(target, sources, moments):
    relative = sources[:3, None, :] - target[:, :, None]
    distance = lax.optimization_barrier(jnp.sum(relative * relative, axis=0)) + SOFT2
    inverse = lax.rsqrt(distance)
    strength = sources[3][None, :] * inverse * inverse * inverse
    near_sum = lax.optimization_barrier(jnp.sum(relative * strength[None], axis=2))
    return GRAV * (near_sum + far_field(target, moments))

def force_item(packed_item):
    return tile_force(packed_item[0], packed_item[1], packed_item[2])

def accelerate(bodies, face_stack, moment_stack, near_local, near_remote, far_list):
    count_tiles = bodies.shape[1]
    tile_size = bodies.shape[2]
    near_slots = face_stack.shape[1]
    slots = face_stack.shape[2]
    moment_levels = moment_stack.shape[1]
    local_src = jnp.take(bodies, near_local, axis=1)
    flat_faces = face_stack.reshape(4, near_slots * slots, tile_size)
    remote_index = (near_remote + (jnp.arange(near_slots, dtype=jnp.int32) * slots)[None, :, None]).reshape(count_tiles, -1)
    remote = jnp.take(flat_faces, remote_index, axis=1)
    sources = jnp.concatenate([local_src, remote], axis=2).reshape(4, count_tiles, -1).transpose(1, 0, 2)
    far_index = (far_list + (jnp.arange(moment_levels, dtype=jnp.int32) * count_tiles)[None, :, None]).reshape(count_tiles, -1)
    picked = jnp.take(moment_stack.reshape(10, moment_levels * count_tiles), far_index, axis=1).transpose(1, 0, 2)
    targets = bodies[:3].transpose(1, 0, 2)
    result = lax.map(force_item, (targets, sources, picked))
    return result.transpose(1, 0, 2)

def reference(offsets, velocities, masses, active, near_local, near_remote, far_list):
    tile_grid = TG
    devices = NPART // (NT * TILE)
    corners = tile_corners(tile_grid)
    position = offsets.reshape(3, devices, NT, TILE).transpose(1, 0, 2, 3) + corners[None, :, :, None]
    velocity = velocities.reshape(3, devices, NT, TILE).transpose(1, 0, 2, 3)
    tile_mass = masses.reshape(devices, NT, TILE)
    weight = active.reshape(devices, NT, TILE).astype(jnp.float32)
    local_lists = near_local.reshape(devices, NT, KL)
    remote_lists = near_remote.reshape(devices, NT, 3, KN)
    far_lists = far_list.reshape(devices, NT, LEVELS, KM)
    z_bits = N_GZ.bit_length() - 1
    y_bits = N_GY.bit_length() - 1
    steps_taken = []
    acceleration = jnp.zeros_like(position)
    for substep in range(SUBSTEPS):
        bodies = jnp.concatenate([position, tile_mass[:, None]], axis=1)

        def device_accel(device):
            own_bodies = bodies[device]
            face_list = [None, None, None]
            moment_list = []
            for level in range(LEVELS):
                partner = jnp.bitwise_xor(device, 1 << level)
                own_bit = jnp.right_shift(device, level) & 1
                cut_axis, place, near_slot = level_place(level, z_bits, y_bits)
                partner_bodies = bodies[partner]
                shift = signed_shift(own_bit, tile_grid * 2 ** place)
                moment_list.append(tile_moments(partner_bodies).at[1 + cut_axis].add(shift))
                if near_slot >= 0:
                    face_coord = jnp.where(own_bit == 1, tile_grid - 1, 0).astype(jnp.int32)
                    face_tiles = jnp.take(partner_bodies, face_index(cut_axis, face_coord, tile_grid), axis=1)
                    face_list[near_slot] = face_tiles.at[cut_axis].add(shift)
            return accelerate(own_bodies, jnp.stack(face_list, axis=1), jnp.stack(moment_list, axis=1), local_lists[device], remote_lists[device], far_lists[device])
        acceleration = lax.map(device_accel, jnp.arange(devices, dtype=jnp.int32))
        magnitude = jnp.sqrt(lax.optimization_barrier(jnp.sum(acceleration * acceleration, axis=1)))
        largest = jnp.max(jnp.where(weight > 0, magnitude, 0.0))
        time_step = ETA / jnp.sqrt(largest + 1e-06)
        velocity = velocity + weight[:, None] * acceleration * time_step
        position = position + weight[:, None] * velocity * time_step
        steps_taken.append(time_step)

    def flatten(values):
        return values.transpose(1, 0, 2, 3).reshape(3, -1)
    return (flatten(position), flatten(velocity), flatten(weight[:, None] * acceleration), jnp.stack(steps_taken))
```

```python
import functools

import jax
import jax.numpy as jnp
from jax import lax
from jax.experimental import pallas as pl
from jax.experimental.pallas import tpu as pltpu
from jax.sharding import PartitionSpec as P

SUBSTEPS = 2
GRAV = 0.02
SOFT2 = 0.0025
ETA = 0.15
AXES = ("gx", "gy", "gz")
F32 = jnp.float32
BF16 = jnp.bfloat16
FAST_GROUPS = 6
STEP = 16


def up8(count):
    return (count + 7) // 8 * 8


def level_place(level, z_bits, y_bits):
    if level < z_bits:
        return (2, level, 0 if level == 0 else -1)
    if level < z_bits + y_bits:
        return (1, level - z_bits, 1 if level == z_bits else -1)
    return (0, level - z_bits - y_bits, 2 if level == z_bits + y_bits else -1)


class Plan:
    def __init__(self, mesh, count_tiles, tile_size, levels, km, kl, kn):
        self.tiles = count_tiles
        self.size = tile_size
        self.rows = up8(count_tiles)
        self.grid = round(count_tiles ** (1 / 3))
        self.face = self.grid * self.grid
        self.levels = levels
        self.km = km
        self.kl = kl
        self.kn = kn
        self.devices = mesh.size
        z_bits = mesh.shape["gz"].bit_length() - 1
        y_bits = mesh.shape["gy"].bit_length() - 1
        x_bits = mesh.shape["gx"].bit_length() - 1
        self.place = [level_place(level, z_bits, y_bits) for level in range(levels)]
        self.near_level = [None] * 3
        for level, (_, _, slot) in enumerate(self.place):
            if slot >= 0:
                self.near_level[slot] = level
        self.frows = up8(3 * self.face)
        self.row_u = self.frows
        self.row_m = 2 * self.frows
        self.row_t = self.row_m + up8(self.face)
        self.near_rows = self.row_t + self.rows
        self.stages = []
        start = 0
        for bits in (z_bits, y_bits, x_bits):
            low = start
            while low < start + bits:
                top = min(low + 2, start + bits)
                self.stages.append(list(range(low, top)))
                low = top
            start += bits


def lane_sum(values):
    return jnp.sum(values, axis=1, keepdims=True)


def split3(values):
    high = values.astype(BF16)
    rest = values - high.astype(F32)
    middle = rest.astype(BF16)
    low = (rest - middle.astype(F32)).astype(BF16)
    return high, middle, low


def dot_nt(left, right):
    return lax.dot_general(left, right, (((1,), (1,)), ((), ())), preferred_element_type=F32)


def dot_nn(left, right):
    return lax.dot_general(left, right, (((1,), (0,)), ((), ())), preferred_element_type=F32)


PAIRS = ((0, 0), (1, 1), (2, 2), (0, 1), (0, 2), (1, 2))


def moment_table(mass, parts):
    shape = mass.shape
    lane = lax.broadcasted_iota(jnp.int32, shape, 1)
    total = lane_sum(mass)
    columns = [(0, total)]
    rel = []
    for k, part in enumerate(parts):
        line = []
        for c in range(3):
            center = lane_sum(mass * part[c]) / total
            columns.append((k * STEP + 1 + c, center))
            line.append(part[c] - center)
        rel.append(line)
    weighted = [[mass * line[c] for c in range(3)] for line in rel]
    count = len(parts)
    for k in range(2 * count - 1):
        second = []
        for a, b in PAIRS:
            term = None
            for i in range(count):
                j = k - i
                if 0 <= j < count:
                    item = weighted[i][a] * rel[j][b]
                    term = item if term is None else term + item
            second.append(lane_sum(term))
        trace = second[0] + second[1] + second[2]
        for q in range(6):
            value = 3.0 * second[q] - trace if q < 3 else 3.0 * second[q]
            columns.append((k * STEP + 4 + q, value))
    table = jnp.zeros(shape, F32)
    for where, value in columns:
        table = jnp.where(lane == where, value, table)
    return table


def device_bits(levels):
    device = lax.axis_index(AXES)
    return [jnp.right_shift(device, level) & 1 for level in range(levels)]


def face_rows(plan, slot, bit):
    cut = 2 - slot
    grid = plan.grid
    strides = (grid * grid, grid, 1)
    others = [axis for axis in range(3) if axis != cut]
    coord = jnp.where(bit == 1, 0, grid - 1)
    base = coord * strides[cut]
    return [
        base + s // grid * strides[others[0]] + s % grid * strides[others[1]]
        for s in range(plan.face)
    ]


def first_kernel(plan, off_ref, vel_ref, mass_ref, act_ref, base_ref, mom_ref, *near_refs):
    tiles, rows, size, grid = plan.tiles, plan.rows, plan.size, plan.grid
    tile = lax.broadcasted_iota(jnp.int32, (rows, size), 0)
    base_ref[...] = jnp.zeros(base_ref.shape, F32)
    for t in range(tiles):
        lanes = pl.ds(t * size, size)
        for c in range(3):
            base_ref[c, pl.ds(t, 1), :] = off_ref[pl.ds(c, 1), lanes]
            base_ref[4 + c, pl.ds(t, 1), :] = vel_ref[pl.ds(c, 1), lanes]
    base_ref[3, pl.ds(0, tiles), :] = mass_ref[...]
    base_ref[7, pl.ds(0, tiles), :] = act_ref[...].astype(F32)
    corners = (tile // (grid * grid), tile // grid % grid, tile % grid)
    inside = tile < tiles
    act = base_ref[7]
    position = []
    for c in range(3):
        value = jnp.where(inside, base_ref[c] + corners[c].astype(F32), 0.0)
        base_ref[c] = value
        position.append(value)
        base_ref[4 + c] = base_ref[4 + c] * act
    mass = jnp.where(inside, base_ref[3], 1.0)
    base_ref[3] = mass
    table = moment_table(mass, [position])
    mom_ref[...] = table
    bits = device_bits(plan.levels)
    for slot, ref in enumerate(near_refs):
        ref[pl.ds(plan.row_t, rows), :] = table
        for s, row in enumerate(face_rows(plan, slot, bits[plan.near_level[slot]])):
            for c in range(3):
                ref[pl.ds(c * plan.face + s, 1), :] = base_ref[c, pl.ds(row, 1), :]
                ref[pl.ds(plan.row_u + c * plan.face + s, 1), :] = base_ref[4 + c, pl.ds(row, 1), :]
            ref[pl.ds(plan.row_m + s, 1), :] = base_ref[3, pl.ds(row, 1), :]


def far_field(plan, far_ref, tables, target):
    rows, size = plan.rows, plan.size
    cell = lax.broadcasted_iota(jnp.int32, (rows, rows), 1)
    total = [jnp.zeros((rows, size), F32) for _ in range(3)]
    for level in range(plan.levels):
        parts = split3(tables[level])
        for k in range(plan.km):
            where = level * plan.km + k
            pick = jnp.where(far_ref[:, pl.ds(where, 1)] == cell, 1.0, 0.0).astype(BF16)
            got = dot_nn(pick, parts[0]) + dot_nn(pick, parts[1]) + dot_nn(pick, parts[2])
            q = [jnp.broadcast_to(got[:, p : p + 1], (rows, size)) for p in range(10)]
            r = [target[c] - q[1 + c] for c in range(3)]
            inverse = lax.rsqrt(r[0] * r[0] + r[1] * r[1] + r[2] * r[2] + SOFT2)
            inverse_sq = inverse * inverse
            cube = inverse * inverse_sq
            fifth = cube * inverse_sq
            dot = [
                q[4] * r[0] + q[7] * r[1] + q[8] * r[2],
                q[7] * r[0] + q[5] * r[1] + q[9] * r[2],
                q[8] * r[0] + q[9] * r[1] + q[6] * r[2],
            ]
            form = r[0] * dot[0] + r[1] * dot[1] + r[2] * dot[2]
            scale = q[0] * cube + 2.5 * form * (fifth * inverse_sq)
            for c in range(3):
                total[c] = total[c] + (dot[c] * fifth - scale * r[c])
    return total


def near_field(plan, list_ref, src_ref, face_ref, rank_ref, row_ref, comp_ref, part_ref):
    tiles, size = plan.tiles, plan.size
    kl, kn = plan.kl, plan.kn
    per_tile = kl + 3 * kn
    fast = FAST_GROUPS * 8
    last = tiles - 1

    def one_hot(t, first, count):
        slot = lax.broadcasted_iota(jnp.int32, (count, size), 0).astype(F32) + first
        return rank_ref[pl.ds(t, 1), :] == slot

    def compact(t, first, count):
        pick = jnp.where(one_hot(t, first, count), 1.0, 0.0).astype(BF16)
        sub = lax.broadcasted_iota(jnp.int32, (8, size), 0)
        own = jnp.where(
            sub == 0,
            src_ref[0, pl.ds(t, 1), :],
            jnp.where(sub == 1, src_ref[1, pl.ds(t, 1), :], src_ref[2, pl.ds(t, 1), :]),
        )
        high, middle, low = split3(own)
        return dot_nt(pick, high) + dot_nt(pick, middle) + dot_nt(pick, low)

    def source_rows(t):
        found = []
        for s in range(per_tile):
            index = list_ref[t * per_tile + s]
            if s < kl:
                found.append([src_ref[c, pl.ds(index, 1), :] for c in range(4)])
            else:
                slot = (s - kl) // kn
                found.append([face_ref[slot, c, pl.ds(index, 1), :] for c in range(4)])
        return found

    def pair_sums(packed, sources):
        here = [jnp.broadcast_to(packed[:, c : c + 1], (8, size)) for c in range(3)]
        sums = None
        for source in sources:
            r = [source[c] - here[c] for c in range(3)]
            inverse = lax.rsqrt(r[0] * r[0] + r[1] * r[1] + r[2] * r[2] + SOFT2)
            strength = source[3] * inverse * (inverse * inverse)
            new = [r[c] * strength for c in range(3)]
            sums = new if sums is None else [sums[c] + new[c] for c in range(3)]
        return sums

    def scatter(t):
        out = [None] * 3
        for g in range(FAST_GROUPS):
            mask = one_hot(t, g * 8, 8)
            for c in range(3):
                column = lane_sum(part_ref[t, g, c])
                value = jnp.where(mask, column, 0.0)
                out[c] = value if out[c] is None else out[c] + value
        for c in range(3):
            row_ref[c, pl.ds(t, 1), :] = jnp.sum(out[c], axis=0, keepdims=True)

    def force(t):
        sources = source_rows(t)
        for g in range(FAST_GROUPS):
            sums = pair_sums(comp_ref[t, pl.ds(g * 8, 8), :], sources)
            for c in range(3):
                part_ref[t, g, c] = sums[c]

    comp_ref[0, :, pl.ds(0, 8)] = compact(0, 0, fast)

    def body(t, carry):
        scatter(jnp.maximum(t - 1, 0))
        force(t)
        after = jnp.minimum(t + 1, last)
        comp_ref[after, :, pl.ds(0, 8)] = compact(after, 0, fast)
        return carry

    lax.fori_loop(0, tiles, body, 0)
    scatter(last)

    @pl.when(list_ref[tiles * per_tile + tiles] > fast)
    def _():
        def tile_rest(t, carry):
            def group(g, inner):
                packed = compact(t, g * 8, 8)
                sums = pair_sums(packed, source_rows(t))
                mask = one_hot(t, g * 8, 8)
                for c in range(3):
                    value = jnp.where(mask, lane_sum(sums[c]), 0.0)
                    old = row_ref[c, pl.ds(t, 1), :]
                    row_ref[c, pl.ds(t, 1), :] = old + jnp.sum(value, axis=0, keepdims=True)
                return inner

            groups = (list_ref[tiles * per_tile + t] + 7) // 8
            lax.fori_loop(FAST_GROUPS, groups, group, 0)
            return carry

        lax.fori_loop(0, tiles, tile_rest, 0)


def shift_of(plan, level, bit):
    _, place, _ = plan.place[level]
    span = float(plan.grid * 2**place)
    return jnp.where(bit == 0, span, -span).astype(F32)


def forces(plan, act, target, tables, list_ref, far_ref, src_ref, face_ref, scratch):
    rank_ref, row_ref, comp_ref, part_ref = scratch
    rows, size = plan.rows, plan.size
    below = lax.broadcasted_iota(jnp.int32, (size, size), 0) < lax.broadcasted_iota(
        jnp.int32, (size, size), 1
    )
    rank = dot_nn(act.astype(BF16), jnp.where(below, 1.0, 0.0).astype(BF16))
    rank_ref[...] = jnp.where(act > 0, rank, -1.0)
    row_ref[...] = jnp.zeros(row_ref.shape, F32)
    far = far_field(plan, far_ref, tables, target)
    near_field(plan, list_ref, src_ref, face_ref, rank_ref, row_ref, comp_ref, part_ref)
    return [act * (GRAV * (row_ref[c] + far[c])) for c in range(3)]


def lane_row(plan, level, bit):
    cut, _, _ = plan.place[level]
    lane = lax.broadcasted_iota(jnp.int32, (1, plan.size), 1)
    return jnp.where(lane == 1 + cut, shift_of(plan, level, bit), 0.0)


def square_row(acc):
    square = acc[0] * acc[0] + acc[1] * acc[1] + acc[2] * acc[2]
    return jnp.max(square, axis=0, keepdims=True)


def time_step_of(square):
    return ETA / jnp.sqrt(jnp.sqrt(square) + 1e-06)


def second_kernel(plan, *refs):
    base_ref, list_ref, far_ref = refs[:3]
    near_refs = refs[3:6]
    extra = plan.levels - 3
    moment_refs = refs[6 : 6 + extra]
    acc_ref, max_ref, mom_ref = refs[6 + extra : 9 + extra]
    send_refs = refs[9 + extra : 12 + extra]
    src_ref, face_ref, *scratch = refs[12 + extra :]
    rows = plan.rows
    bits = device_bits(plan.levels)
    src_ref[...] = base_ref[pl.ds(0, 4)]
    tables = []
    others = list(moment_refs)
    for level in range(plan.levels):
        slot = plan.place[level][2]
        table = near_refs[slot][pl.ds(plan.row_t, rows), :] if slot >= 0 else others.pop(0)[...]
        tables.append(table + lane_row(plan, level, bits[level]))
    face = plan.face
    for slot in range(3):
        level = plan.near_level[slot]
        cut = plan.place[level][0]
        for c in range(3):
            value = near_refs[slot][pl.ds(c * face, face), :]
            if c == cut:
                value = value + shift_of(plan, level, bits[level])
            face_ref[slot, c, pl.ds(0, face), :] = value
        face_ref[slot, 3, pl.ds(0, face), :] = near_refs[slot][pl.ds(plan.row_m, face), :]
    act = base_ref[7]
    position = [base_ref[c] for c in range(3)]
    acc = forces(plan, act, position, tables, list_ref, far_ref, src_ref, face_ref, scratch)
    for c in range(3):
        acc_ref[c] = acc[c]
    max_ref[...] = square_row(acc)
    table = moment_table(base_ref[3], [position, [base_ref[4 + c] for c in range(3)], acc])
    mom_ref[...] = table
    for slot, ref in enumerate(send_refs):
        ref[pl.ds(plan.frows, rows), :] = table
        for s, row in enumerate(face_rows(plan, slot, bits[plan.near_level[slot]])):
            for c in range(3):
                ref[pl.ds(c * face + s, 1), :] = acc_ref[c, pl.ds(row, 1), :]


def third_kernel(plan, *refs):
    base_ref, list_ref, far_ref, acc_ref, max_ref = refs[:5]
    near_refs = refs[5:8]
    send_refs = refs[8:11]
    extra = plan.levels - 3
    moment_refs = refs[11 : 11 + extra]
    pos_ref, out_ref, square_ref, step_ref = refs[11 + extra : 15 + extra]
    src_ref, face_ref, moved_ref, *scratch = refs[15 + extra :]
    rows, size = plan.rows, plan.size
    bits = device_bits(plan.levels)
    step = time_step_of(jnp.max(max_ref[...], axis=(0, 1), keepdims=True))
    step_ref[...] = jnp.broadcast_to(step, step_ref.shape)
    dt = jnp.broadcast_to(step, (8, size))
    wide = jnp.broadcast_to(step, (rows, size))
    position = []
    for c in range(3):
        moved = base_ref[c] + (base_ref[4 + c] + acc_ref[c] * wide) * wide
        pos_ref[c] = moved
        src_ref[c] = moved
        position.append(moved)
    src_ref[3] = base_ref[3]
    lane = lax.broadcasted_iota(jnp.int32, (rows, size), 1)
    tables = []
    others = list(moment_refs)
    for level in range(plan.levels):
        slot = plan.place[level][2]
        table = send_refs[slot][pl.ds(plan.frows, rows), :] if slot >= 0 else others.pop(0)[...]
        total = None
        for k in range(4, -1, -1):
            part = pltpu.roll(table, size - k * STEP, 1) if k else table
            total = part if total is None else total * wide + part
        tables.append(jnp.where(lane < 10, total, 0.0) + lane_row(plan, level, bits[level]))
    face = plan.face
    frows = plan.frows
    fwide = jnp.broadcast_to(step, (frows, size))
    for slot in range(3):
        level = plan.near_level[slot]
        cut = plan.place[level][0]
        near = near_refs[slot]
        moved_ref[...] = (
            near[pl.ds(0, frows), :]
            + (near[pl.ds(plan.row_u, frows), :] + send_refs[slot][pl.ds(0, frows), :] * fwide)
            * fwide
        )
        for c in range(3):
            value = moved_ref[pl.ds(c * face, face), :]
            if c == cut:
                value = value + shift_of(plan, level, bits[level])
            face_ref[slot, c, pl.ds(0, face), :] = value
        face_ref[slot, 3, pl.ds(0, face), :] = near[pl.ds(plan.row_m, face), :]
    act = base_ref[7]
    acc = forces(plan, act, position, tables, list_ref, far_ref, src_ref, face_ref, scratch)
    for c in range(3):
        out_ref[c] = acc[c]
    square_ref[...] = square_row(acc)


def last_kernel(plan, max_ref, vel_ref, base_ref, pos_ref, first_ref, acc_ref, step_ref,
                pos_out, vel_out, acc_out, steps_out, work_ref):
    rows, size = plan.rows, plan.size
    second = time_step_of(jnp.max(max_ref[...], axis=(0, 1), keepdims=True))
    one = step_ref[...]
    lane = lax.broadcasted_iota(jnp.int32, (1, size), 1)
    steps_out[...] = jnp.where(lane == 0, one, second)
    first = jnp.broadcast_to(one[:, :1], (rows, size))
    wide = jnp.broadcast_to(second, (rows, size))
    for c in range(3):
        kick = acc_ref[c] * wide
        before = first_ref[c] * first
        work_ref[0, c] = pos_ref[c] + (base_ref[4 + c] + before + kick) * wide
        work_ref[1, c] = before
        work_ref[2, c] = kick
    for t in range(plan.tiles):
        lanes = pl.ds(t * size, size)
        for c in range(3):
            pos_out[pl.ds(c, 1), lanes] = work_ref[0, c, pl.ds(t, 1), :]
            vel_out[pl.ds(c, 1), lanes] = (
                vel_ref[pl.ds(c, 1), lanes] + work_ref[1, c, pl.ds(t, 1), :]
            ) + work_ref[2, c, pl.ds(t, 1), :]
            acc_out[pl.ds(c, 1), lanes] = acc_ref[c, pl.ds(t, 1), :]


def vmem():
    return pl.BlockSpec(memory_space=pltpu.VMEM)


def smem():
    return pl.BlockSpec(memory_space=pltpu.SMEM)


def call(kernel, outs, scratch, specs, name):
    return pl.pallas_call(
        kernel,
        out_shape=[jax.ShapeDtypeStruct(shape, F32) for shape in outs],
        in_specs=specs,
        out_specs=[vmem() for _ in outs],
        scratch_shapes=[pltpu.VMEM(shape, F32) for shape in scratch],
        name=name,
    )


def exchange(plan, block, bits):
    flip = sum(1 << bit for bit in bits)
    return lax.ppermute(block, AXES, [(i, i ^ flip) for i in range(plan.devices)])


def body(mesh, offsets, velocities, masses, active, near_local, near_remote, far_list):
    tiles, kl = near_local.shape
    kn = near_remote.shape[2]
    levels, km = far_list.shape[1:]
    size = masses.shape[0] // tiles
    plan = Plan(mesh, tiles, size, levels, km, kl, kn)
    rows, near_rows = plan.rows, plan.near_rows
    whole = (3, rows, size)
    extra = levels - 3
    active2 = active.reshape(tiles, size)
    base, moments, *near = call(
        functools.partial(first_kernel, plan),
        [(8, rows, size), (rows, size)] + [(near_rows, size)] * 3,
        [],
        [vmem()] * 4,
        "first",
    )(offsets, velocities, masses.reshape(tiles, size), active2)

    got_near = [None] * 3
    got_far = []
    for slot in range(3):
        got_near[slot] = exchange(plan, near[slot], [plan.near_level[slot]])
    for level in range(levels):
        if plan.place[level][2] < 0:
            got_far.append(exchange(plan, moments, [level]))

    counts = jnp.sum(active2, axis=1)
    lists = jnp.concatenate(
        [
            jnp.concatenate([near_local, near_remote.reshape(tiles, 3 * kn)], axis=1).reshape(-1),
            counts,
            jnp.max(counts)[None],
        ]
    )
    far_ids = far_list.reshape(tiles, levels * km)
    far_ids = jnp.concatenate(
        [far_ids, jnp.zeros((rows - tiles, levels * km), jnp.int32)], axis=0
    )
    fast = FAST_GROUPS * 8
    scratch = [
        (4, rows, size),
        (3, 4, up8(plan.face), size),
        (rows, size),
        whole,
        (tiles, fast, size),
        (tiles, FAST_GROUPS, 3, 8, size),
    ]
    send_rows = plan.frows + rows
    acc, square, table, *send = call(
        functools.partial(second_kernel, plan),
        [whole, (1, size), (rows, size)] + [(send_rows, size)] * 3,
        scratch,
        [vmem(), smem()] + [vmem()] * (1 + levels),
        "second",
    )(base, lists, far_ids, *got_near, *got_far)

    got_send = [None] * 3
    got_table = {}
    best = square
    for stage in plan.stages:
        flips = [[bit] for bit in stage] + ([stage] if len(stage) > 1 else [])
        seen = [best]
        for flip in flips:
            slot = plan.place[flip[0]][2] if len(flip) == 1 else -1
            if len(flip) > 1:
                seen.append(exchange(plan, best, flip))
                continue
            data = send[slot] if slot >= 0 else table
            there = exchange(plan, jnp.concatenate([data, best], axis=0), flip)
            seen.append(there[data.shape[0] :])
            if slot >= 0:
                got_send[slot] = there
            else:
                got_table[flip[0]] = there
        best = functools.reduce(jnp.maximum, seen)
    moved, acc2, square2, step = call(
        functools.partial(third_kernel, plan),
        [whole, whole, (1, size), (1, size)],
        scratch[:2] + [(plan.frows, size)] + scratch[2:],
        [vmem(), smem()] + [vmem()] * (3 + 3 + 3 + extra),
        "third",
    )(
        base, lists, far_ids, acc, best, *got_near, *got_send,
        *[got_table[level][:rows] for level in range(levels) if plan.place[level][2] < 0],
    )
    spread = jnp.broadcast_to(square2[None], (plan.devices, 1, size))
    everyone = lax.all_to_all(spread, AXES, 0, 0).reshape(plan.devices, size)
    pos, vel, out, steps = call(
        functools.partial(last_kernel, plan),
        [offsets.shape, offsets.shape, offsets.shape, (1, size)],
        [(3, 3, rows, size)],
        [vmem()] * 7,
        "last",
    )(everyone, velocities, base, moved, acc, acc2, step)
    return pos, vel, out, steps[0, :SUBSTEPS]


def solution(mesh):
    parts = P(None, AXES)
    return jax.shard_map(
        functools.partial(body, mesh),
        mesh=mesh,
        in_specs=(parts, parts, P(AXES), P(AXES), P(AXES, None), P(AXES, None, None), P(AXES, None, None)),
        out_specs=(parts, parts, parts, P()),
        check_vma=False,
    )
```

```python
import functools

import jax
import jax.numpy as jnp
from jax import lax
from jax.experimental import pallas as pl
from jax.experimental.pallas import tpu as pltpu
from jax.sharding import PartitionSpec as P

SUBSTEPS = 2
GRAV = 0.02
SOFT2 = 0.0025
ETA = 0.15
AXES = ("gx", "gy", "gz")
F32 = jnp.float32
BF16 = jnp.bfloat16
FAST_GROUPS = 6
VMEM_BYTES = 16 * 2**20
STEP = 16


def up8(count):
    return (count + 7) // 8 * 8


def level_place(level, z_bits, y_bits):
    if level < z_bits:
        return (2, level, 0 if level == 0 else -1)
    if level < z_bits + y_bits:
        return (1, level - z_bits, 1 if level == z_bits else -1)
    return (0, level - z_bits - y_bits, 2 if level == z_bits + y_bits else -1)


class Plan:
    def __init__(self, mesh, count_tiles, tile_size, levels, km, kl, kn):
        self.tiles = count_tiles
        self.size = tile_size
        self.rows = up8(count_tiles)
        self.grid = round(count_tiles ** (1 / 3))
        self.face = self.grid * self.grid
        self.levels = levels
        self.km = km
        self.kl = kl
        self.kn = kn
        self.devices = mesh.size
        z_bits = mesh.shape["gz"].bit_length() - 1
        y_bits = mesh.shape["gy"].bit_length() - 1
        x_bits = mesh.shape["gx"].bit_length() - 1
        self.place = [level_place(level, z_bits, y_bits) for level in range(levels)]
        self.near_level = [None] * 3
        for level, (_, _, slot) in enumerate(self.place):
            if slot >= 0:
                self.near_level[slot] = level
        self.frows = up8(3 * self.face)
        self.row_u = self.frows
        self.row_m = 2 * self.frows
        self.row_t = self.row_m + up8(self.face)
        self.near_rows = self.row_t + self.rows
        self.stages = []
        start = 0
        for bits in (z_bits, y_bits, x_bits):
            low = start
            while low < start + bits:
                top = min(low + 2, start + bits)
                self.stages.append(list(range(low, top)))
                low = top
            start += bits


def lane_sum(values):
    return jnp.sum(values, axis=1, keepdims=True)


def split3(values):
    high = values.astype(BF16)
    rest = values - high.astype(F32)
    middle = rest.astype(BF16)
    low = (rest - middle.astype(F32)).astype(BF16)
    return high, middle, low


def dot_nt(left, right):
    return lax.dot_general(left, right, (((1,), (1,)), ((), ())), preferred_element_type=F32)


def dot_nn(left, right):
    return lax.dot_general(left, right, (((1,), (0,)), ((), ())), preferred_element_type=F32)


PAIRS = ((0, 0), (1, 1), (2, 2), (0, 1), (0, 2), (1, 2))


def moment_table(mass, parts):
    shape = mass.shape
    lane = lax.broadcasted_iota(jnp.int32, shape, 1)
    total = lane_sum(mass)
    columns = [(0, total)]
    rel = []
    for k, part in enumerate(parts):
        line = []
        for c in range(3):
            center = lane_sum(mass * part[c]) / total
            columns.append((k * STEP + 1 + c, center))
            line.append(part[c] - center)
        rel.append(line)
    weighted = [[mass * line[c] for c in range(3)] for line in rel]
    count = len(parts)
    for k in range(2 * count - 1):
        second = []
        for a, b in PAIRS:
            term = None
            for i in range(count):
                j = k - i
                if 0 <= j < count:
                    item = weighted[i][a] * rel[j][b]
                    term = item if term is None else term + item
            second.append(lane_sum(term))
        trace = second[0] + second[1] + second[2]
        for q in range(6):
            value = 3.0 * second[q] - trace if q < 3 else 3.0 * second[q]
            columns.append((k * STEP + 4 + q, value))
    table = jnp.zeros(shape, F32)
    for where, value in columns:
        table = jnp.where(lane == where, value, table)
    return table


def device_bits(levels):
    device = lax.axis_index(AXES)
    return [jnp.right_shift(device, level) & 1 for level in range(levels)]


def face_rows(plan, slot, bit):
    cut = 2 - slot
    grid = plan.grid
    strides = (grid * grid, grid, 1)
    others = [axis for axis in range(3) if axis != cut]
    coord = jnp.where(bit == 1, 0, grid - 1)
    base = coord * strides[cut]
    return [
        base + s // grid * strides[others[0]] + s % grid * strides[others[1]]
        for s in range(plan.face)
    ]


def first_kernel(plan, *refs):
    ins, (base_ref, mom_ref, id_ref), near_refs = refs[:5], refs[5:8], refs[8:11]
    buffers, sems = refs[11:16], refs[16]
    copies = [pltpu.make_async_copy(ins[i], buffers[i], sems.at[i]) for i in range(5)]
    for copy in copies:
        copy.start()
    for copy in copies:
        copy.wait()
    off_ref, vel_ref, mass_ref, act_ref, far_ref = buffers
    tiles, rows, size, grid = plan.tiles, plan.rows, plan.size, plan.grid
    tile = lax.broadcasted_iota(jnp.int32, (rows, size), 0)
    base_ref[...] = jnp.zeros(base_ref.shape, F32)
    for t in range(tiles):
        lanes = pl.ds(t * size, size)
        for c in range(3):
            base_ref[c, pl.ds(t, 1), :] = off_ref[pl.ds(c, 1), lanes]
            base_ref[4 + c, pl.ds(t, 1), :] = vel_ref[pl.ds(c, 1), lanes]
    base_ref[3, pl.ds(0, tiles), :] = mass_ref[...]
    base_ref[7, pl.ds(0, tiles), :] = act_ref[...].astype(F32)
    corners = (tile // (grid * grid), tile // grid % grid, tile % grid)
    inside = tile < tiles
    act = base_ref[7]
    position = []
    for c in range(3):
        value = jnp.where(inside, base_ref[c] + corners[c].astype(F32), 0.0)
        base_ref[c] = value
        position.append(value)
    mass = jnp.where(inside, base_ref[3], 1.0)
    base_ref[3] = mass
    table = moment_table(mass, [position])
    mom_ref[...] = table
    lists = plan.levels * plan.km
    flat = jnp.concatenate(
        [far_ref[level].astype(F32) for level in range(plan.levels)]
        + [jnp.zeros((up8(lists) - lists, tiles), F32)] * (lists % 8 > 0),
        axis=0,
    )
    id_ref[pl.ds(0, tiles), pl.ds(0, up8(lists))] = jnp.transpose(flat).astype(jnp.int32)
    bits = device_bits(plan.levels)
    for slot, ref in enumerate(near_refs):
        ref[pl.ds(plan.row_t, rows), :] = table
        for s, row in enumerate(face_rows(plan, slot, bits[plan.near_level[slot]])):
            for c in range(3):
                ref[pl.ds(c * plan.face + s, 1), :] = base_ref[c, pl.ds(row, 1), :]
                ref[pl.ds(plan.row_u + c * plan.face + s, 1), :] = (
                    base_ref[4 + c, pl.ds(row, 1), :] * base_ref[7, pl.ds(row, 1), :]
                )
            ref[pl.ds(plan.row_m + s, 1), :] = base_ref[3, pl.ds(row, 1), :]


def far_field(plan, far_ref, tables, target):
    rows, size = plan.rows, plan.size
    cell = lax.broadcasted_iota(jnp.int32, (rows, rows), 1)
    far_ids = far_ref[...]
    total = [jnp.zeros((rows, size), F32) for _ in range(3)]
    for level in range(plan.levels):
        parts = split3(tables[level])
        for k in range(plan.km):
            where = level * plan.km + k
            pick = jnp.where(far_ids[:, where : where + 1] == cell, 1.0, 0.0).astype(BF16)
            got = dot_nn(pick, parts[0]) + dot_nn(pick, parts[1]) + dot_nn(pick, parts[2])
            q = [jnp.broadcast_to(got[:, p : p + 1], (rows, size)) for p in range(10)]
            r = [target[c] - q[1 + c] for c in range(3)]
            inverse = lax.rsqrt(r[0] * r[0] + r[1] * r[1] + r[2] * r[2] + SOFT2)
            inverse_sq = inverse * inverse
            cube = inverse * inverse_sq
            fifth = cube * inverse_sq
            dot = [
                q[4] * r[0] + q[7] * r[1] + q[8] * r[2],
                q[7] * r[0] + q[5] * r[1] + q[9] * r[2],
                q[8] * r[0] + q[9] * r[1] + q[6] * r[2],
            ]
            form = r[0] * dot[0] + r[1] * dot[1] + r[2] * dot[2]
            scale = q[0] * cube + 2.5 * form * (fifth * inverse_sq)
            for c in range(3):
                total[c] = total[c] + (dot[c] * fifth - scale * r[c])
    return total


def near_field(plan, list_ref, src_ref, face_ref, rank_ref, row_ref, comp_ref, part_ref):
    tiles, size = plan.tiles, plan.size
    kl, kn = plan.kl, plan.kn
    per_tile = kl + 3 * kn
    fast = FAST_GROUPS * 8
    last = tiles - 1

    def one_hot(t, first, count):
        slot = lax.broadcasted_iota(jnp.int32, (count, size), 0).astype(F32) + first
        return rank_ref[pl.ds(t, 1), :] == slot

    def compact(t, first, count):
        pick = jnp.where(one_hot(t, first, count), 1.0, 0.0).astype(BF16)
        sub = lax.broadcasted_iota(jnp.int32, (8, size), 0)
        own = jnp.where(
            sub == 0,
            src_ref[0, pl.ds(t, 1), :],
            jnp.where(sub == 1, src_ref[1, pl.ds(t, 1), :], src_ref[2, pl.ds(t, 1), :]),
        )
        high, middle, low = split3(own)
        return dot_nt(pick, high) + dot_nt(pick, middle) + dot_nt(pick, low)

    def source_rows(t):
        found = []
        for s in range(per_tile):
            if s < kl:
                index = list_ref[0][s, t]
                found.append([src_ref[c, pl.ds(index, 1), :] for c in range(4)])
            else:
                slot = (s - kl) // kn
                index = list_ref[1][slot, (s - kl) % kn, t]
                found.append([face_ref[slot, c, pl.ds(index, 1), :] for c in range(4)])
        return found

    def pair_sums(packed, sources):
        here = [jnp.broadcast_to(packed[:, c : c + 1], (8, size)) for c in range(3)]
        sums = None
        for source in sources:
            r = [source[c] - here[c] for c in range(3)]
            inverse = lax.rsqrt(r[0] * r[0] + r[1] * r[1] + r[2] * r[2] + SOFT2)
            strength = source[3] * inverse * (inverse * inverse)
            new = [r[c] * strength for c in range(3)]
            sums = new if sums is None else [sums[c] + new[c] for c in range(3)]
        return sums

    def scatter(t):
        out = [None] * 3
        for g in range(FAST_GROUPS):
            mask = one_hot(t, g * 8, 8)
            for c in range(3):
                column = lane_sum(part_ref[t, g, c])
                value = jnp.where(mask, column, 0.0)
                out[c] = value if out[c] is None else out[c] + value
        for c in range(3):
            row_ref[c, pl.ds(t, 1), :] = jnp.sum(out[c], axis=0, keepdims=True)

    def force(t):
        sources = source_rows(t)
        for g in range(FAST_GROUPS):
            sums = pair_sums(comp_ref[t, pl.ds(g * 8, 8), :], sources)
            for c in range(3):
                part_ref[t, g, c] = sums[c]

    comp_ref[0, :, pl.ds(0, 8)] = compact(0, 0, fast)

    def body(t, carry):
        scatter(jnp.maximum(t - 1, 0))
        force(t)
        after = jnp.minimum(t + 1, last)
        comp_ref[after, :, pl.ds(0, 8)] = compact(after, 0, fast)
        return carry

    lax.fori_loop(0, tiles, body, 0)
    scatter(last)

    @pl.when(jnp.max(rank_ref[...]) >= fast)
    def _():
        def tile_rest(t, carry):
            def group(g, inner):
                packed = compact(t, g * 8, 8)
                sums = pair_sums(packed, source_rows(t))
                mask = one_hot(t, g * 8, 8)
                for c in range(3):
                    value = jnp.where(mask, lane_sum(sums[c]), 0.0)
                    old = row_ref[c, pl.ds(t, 1), :]
                    row_ref[c, pl.ds(t, 1), :] = old + jnp.sum(value, axis=0, keepdims=True)
                return inner

            groups = (jnp.max(rank_ref[pl.ds(t, 1), :]).astype(jnp.int32) + 8) // 8
            lax.fori_loop(FAST_GROUPS, groups, group, 0)
            return carry

        lax.fori_loop(0, tiles, tile_rest, 0)


def shift_of(plan, level, bit):
    _, place, _ = plan.place[level]
    span = float(plan.grid * 2**place)
    return jnp.where(bit == 0, span, -span).astype(F32)


def lists_start(ins, scratch):
    outs, sems = scratch[:2], scratch[2]
    copies = [pltpu.make_async_copy(ins[i], outs[i], sems.at[i]) for i in range(2)]
    for copy in copies:
        copy.start()

    def arrived():
        for copy in copies:
            copy.wait()
        return outs

    return arrived


def forces(plan, act, target, tables, arrived, far_ref, src_ref, face_ref, scratch):
    rank_ref, row_ref, comp_ref, part_ref = scratch
    rows, size = plan.rows, plan.size
    below = lax.broadcasted_iota(jnp.int32, (size, size), 0) < lax.broadcasted_iota(
        jnp.int32, (size, size), 1
    )
    rank = dot_nn(act.astype(BF16), jnp.where(below, 1.0, 0.0).astype(BF16))
    rank_ref[...] = jnp.where(act > 0, rank, -1.0)
    row_ref[...] = jnp.zeros(row_ref.shape, F32)
    far = far_field(plan, far_ref, tables, target)
    near_field(plan, arrived(), src_ref, face_ref, rank_ref, row_ref, comp_ref, part_ref)
    return [act * (GRAV * (row_ref[c] + far[c])) for c in range(3)]


def lane_row(plan, level, bit):
    cut, _, _ = plan.place[level]
    lane = lax.broadcasted_iota(jnp.int32, (1, plan.size), 1)
    return jnp.where(lane == 1 + cut, shift_of(plan, level, bit), 0.0)


def square_row(acc):
    square = acc[0] * acc[0] + acc[1] * acc[1] + acc[2] * acc[2]
    return jnp.max(square, axis=0, keepdims=True)


def time_step_of(square):
    return ETA / jnp.sqrt(jnp.sqrt(square) + 1e-06)


def second_kernel(plan, *refs):
    arrived, refs = lists_start(refs[:2], refs[-10:-7]), refs[2:]
    base_ref, far_ref = refs[:2]
    near_refs = refs[2:5]
    extra = plan.levels - 3
    moment_refs = refs[5 : 5 + extra]
    acc_ref, max_ref, mom_ref = refs[5 + extra : 8 + extra]
    send_refs = refs[8 + extra : 11 + extra]
    src_ref, face_ref, _, *scratch = refs[-7:]
    rows = plan.rows
    bits = device_bits(plan.levels)
    src_ref[...] = base_ref[pl.ds(0, 4)]
    tables = []
    others = list(moment_refs)
    for level in range(plan.levels):
        slot = plan.place[level][2]
        table = near_refs[slot][pl.ds(plan.row_t, rows), :] if slot >= 0 else others.pop(0)[...]
        tables.append(table + lane_row(plan, level, bits[level]))
    face = plan.face
    for slot in range(3):
        level = plan.near_level[slot]
        cut = plan.place[level][0]
        for c in range(3):
            value = near_refs[slot][pl.ds(c * face, face), :]
            if c == cut:
                value = value + shift_of(plan, level, bits[level])
            face_ref[slot, c, pl.ds(0, face), :] = value
        face_ref[slot, 3, pl.ds(0, face), :] = near_refs[slot][pl.ds(plan.row_m, face), :]
    act = base_ref[7]
    position = [base_ref[c] for c in range(3)]
    acc = forces(plan, act, position, tables, arrived, far_ref, src_ref, face_ref, scratch)
    for c in range(3):
        acc_ref[c] = acc[c]
    max_ref[...] = square_row(acc)
    table = moment_table(base_ref[3], [position, [base_ref[4 + c] * act for c in range(3)], acc])
    mom_ref[...] = table
    for slot, ref in enumerate(send_refs):
        ref[pl.ds(plan.frows, rows), :] = table
        for s, row in enumerate(face_rows(plan, slot, bits[plan.near_level[slot]])):
            for c in range(3):
                ref[pl.ds(c * face + s, 1), :] = acc_ref[c, pl.ds(row, 1), :]


def third_kernel(plan, *refs):
    arrived, refs = lists_start(refs[:2], refs[-10:-7]), refs[2:]
    base_ref, far_ref, acc_ref, max_ref = refs[:4]
    near_refs = refs[4:7]
    send_refs = refs[7:10]
    extra = plan.levels - 3
    moment_refs = refs[10 : 10 + extra]
    pos_ref, out_ref, square_ref, step_ref = refs[10 + extra : 14 + extra]
    src_ref, face_ref, moved_ref, *scratch = refs[-7:]
    rows, size = plan.rows, plan.size
    bits = device_bits(plan.levels)
    step = time_step_of(jnp.max(max_ref[...], axis=(0, 1), keepdims=True))
    step_ref[...] = jnp.broadcast_to(step, step_ref.shape)
    dt = jnp.broadcast_to(step, (8, size))
    wide = jnp.broadcast_to(step, (rows, size))
    position = []
    act = base_ref[7]
    for c in range(3):
        moved = base_ref[c] + (base_ref[4 + c] * act + acc_ref[c] * wide) * wide
        pos_ref[c] = moved
        src_ref[c] = moved
        position.append(moved)
    src_ref[3] = base_ref[3]
    lane = lax.broadcasted_iota(jnp.int32, (rows, size), 1)
    tables = []
    others = list(moment_refs)
    for level in range(plan.levels):
        slot = plan.place[level][2]
        table = send_refs[slot][pl.ds(plan.frows, rows), :] if slot >= 0 else others.pop(0)[...]
        total = None
        for k in range(4, -1, -1):
            part = pltpu.roll(table, size - k * STEP, 1) if k else table
            total = part if total is None else total * wide + part
        tables.append(jnp.where(lane < 10, total, 0.0) + lane_row(plan, level, bits[level]))
    face = plan.face
    frows = plan.frows
    fwide = jnp.broadcast_to(step, (frows, size))
    for slot in range(3):
        level = plan.near_level[slot]
        cut = plan.place[level][0]
        near = near_refs[slot]
        moved_ref[...] = (
            near[pl.ds(0, frows), :]
            + (near[pl.ds(plan.row_u, frows), :] + send_refs[slot][pl.ds(0, frows), :] * fwide)
            * fwide
        )
        for c in range(3):
            value = moved_ref[pl.ds(c * face, face), :]
            if c == cut:
                value = value + shift_of(plan, level, bits[level])
            face_ref[slot, c, pl.ds(0, face), :] = value
        face_ref[slot, 3, pl.ds(0, face), :] = near[pl.ds(plan.row_m, face), :]
    acc = forces(plan, act, position, tables, arrived, far_ref, src_ref, face_ref, scratch)
    for c in range(3):
        out_ref[c] = acc[c]
    square_ref[...] = square_row(acc)


def last_kernel(plan, max_ref, base_ref, pos_ref, first_ref, acc_ref, step_ref,
                pos_out, vel_out, acc_out, steps_out, work_ref):
    rows, size = plan.rows, plan.size
    second = time_step_of(jnp.max(max_ref[...], axis=(0, 1), keepdims=True))
    one = step_ref[...]
    steps_out[0] = one[0, 0]
    steps_out[1] = second[0, 0]
    first = jnp.broadcast_to(one[:, :1], (rows, size))
    wide = jnp.broadcast_to(second, (rows, size))
    act = base_ref[7]
    for c in range(3):
        velocity = base_ref[4 + c] + first_ref[c] * first + acc_ref[c] * wide
        work_ref[0, c] = pos_ref[c] + velocity * act * wide
        work_ref[1, c] = velocity
    for t in range(plan.tiles):
        lanes = pl.ds(t * size, size)
        for c in range(3):
            pos_out[pl.ds(c, 1), lanes] = work_ref[0, c, pl.ds(t, 1), :]
            vel_out[pl.ds(c, 1), lanes] = work_ref[1, c, pl.ds(t, 1), :]
            acc_out[pl.ds(c, 1), lanes] = acc_ref[c, pl.ds(t, 1), :]


def vmem():
    return pl.BlockSpec(memory_space=pltpu.VMEM)


def hbm():
    return pl.BlockSpec(memory_space=pltpu.HBM)


def smem():
    return pl.BlockSpec(memory_space=pltpu.SMEM)


def call(kernel, outs, scratch, specs, name, out_specs=None):
    return pl.pallas_call(
        kernel,
        out_shape=outs,
        in_specs=specs,
        out_specs=out_specs or [vmem() for _ in outs],
        scratch_shapes=scratch,
        compiler_params=pltpu.CompilerParams(vmem_limit_bytes=VMEM_BYTES),
        name=name,
    )


def buffers(*shapes):
    return [pltpu.VMEM(shape, F32) for shape in shapes]


def floats(*shapes):
    return [jax.ShapeDtypeStruct(shape, F32) for shape in shapes]


def exchange(plan, block, bits):
    flip = sum(1 << bit for bit in bits)
    return lax.ppermute(block, AXES, [(i, i ^ flip) for i in range(plan.devices)])


def body(mesh, offsets, velocities, masses, active, near_local, near_remote, far_list):
    tiles, kl = near_local.shape
    kn = near_remote.shape[2]
    levels, km = far_list.shape[1:]
    size = masses.shape[0] // tiles
    plan = Plan(mesh, tiles, size, levels, km, kl, kn)
    rows, near_rows = plan.rows, plan.near_rows
    whole = (3, rows, size)
    extra = levels - 3
    base, moments, far_ids, *near = call(
        functools.partial(first_kernel, plan),
        floats((8, rows, size), (rows, size))
        + [jax.ShapeDtypeStruct((rows, size), jnp.int32)]
        + floats(*[(near_rows, size)] * 3),
        buffers(offsets.shape, velocities.shape, (tiles, size))
        + [
            pltpu.VMEM((tiles, size), jnp.int32),
            pltpu.VMEM((levels, km, tiles), jnp.int32),
            pltpu.SemaphoreType.DMA((5,)),
        ],
        [hbm()] * 5,
        "first",
    )(
        offsets,
        velocities,
        masses.reshape(tiles, size),
        active.reshape(tiles, size),
        jnp.transpose(far_list, (1, 2, 0)),
    )

    got_near = [None] * 3
    got_far = []
    for slot in range(3):
        got_near[slot] = exchange(plan, near[slot], [plan.near_level[slot]])
    for level in range(levels):
        if plan.place[level][2] < 0:
            got_far.append(exchange(plan, moments, [level]))

    lists = (jnp.transpose(near_local), jnp.transpose(near_remote, (1, 2, 0)))
    fast = FAST_GROUPS * 8
    scratch = [
        pltpu.SMEM((kl, tiles), jnp.int32),
        pltpu.SMEM((3, kn, tiles), jnp.int32),
        pltpu.SemaphoreType.DMA((2,)),
    ] + buffers(
        (4, rows, size),
        (3, 4, up8(plan.face), size),
        (plan.frows, size),
        (rows, size),
        whole,
        (tiles, fast, size),
        (tiles, FAST_GROUPS, 3, 8, size),
    )
    send_rows = plan.frows + rows
    acc, square, table, *send = call(
        functools.partial(second_kernel, plan),
        floats(whole, (1, size), (rows, size), *[(send_rows, size)] * 3),
        scratch,
        [hbm(), hbm()] + [vmem()] * (2 + levels),
        "second",
    )(*lists, base, far_ids, *got_near, *got_far)

    got_send = [None] * 3
    got_table = {}
    best = square
    for stage in plan.stages:
        flips = [[bit] for bit in stage] + ([stage] if len(stage) > 1 else [])
        seen = [best]
        for flip in flips:
            slot = plan.place[flip[0]][2] if len(flip) == 1 else -1
            if len(flip) > 1:
                seen.append(exchange(plan, best, flip))
                continue
            data = send[slot] if slot >= 0 else table
            there = exchange(plan, jnp.concatenate([data, best], axis=0), flip)
            seen.append(there[data.shape[0] :])
            if slot >= 0:
                got_send[slot] = there
            else:
                got_table[flip[0]] = there
        best = functools.reduce(jnp.maximum, seen)
    moved, acc2, square2, step = call(
        functools.partial(third_kernel, plan),
        floats(whole, whole, (1, size), (1, size)),
        scratch,
        [hbm(), hbm()] + [vmem()] * (4 + 3 + 3 + extra),
        "third",
    )(
        *lists, base, far_ids, acc, best, *got_near, *got_send,
        *[got_table[level][:rows] for level in range(levels) if plan.place[level][2] < 0],
    )
    spread = jnp.broadcast_to(square2[None], (plan.devices, 1, size))
    everyone = lax.all_to_all(spread, AXES, 0, 0).reshape(plan.devices, size)
    pos, vel, out, steps = call(
        functools.partial(last_kernel, plan),
        floats(offsets.shape, offsets.shape, offsets.shape, (SUBSTEPS,)),
        buffers((2, 3, rows, size)),
        [vmem()] * 6,
        "last",
        [vmem(), vmem(), vmem(), smem()],
    )(everyone, base, moved, acc, acc2, step)
    return pos, vel, out, steps


def solution(mesh):
    parts = P(None, AXES)
    return jax.shard_map(
        functools.partial(body, mesh),
        mesh=mesh,
        in_specs=(parts, parts, P(AXES), P(AXES), P(AXES, None), P(AXES, None, None), P(AXES, None, None)),
        out_specs=(parts, parts, parts, P()),
        check_vma=False,
    )
```

```python
import functools

import jax
import jax.numpy as jnp
from jax import lax
from jax.experimental import pallas as pl
from jax.experimental.pallas import tpu as pltpu
from jax.sharding import PartitionSpec as P

SUBSTEPS = 2
GRAV = 0.02
SOFT2 = 0.0025
ETA = 0.15
AXES = ("gx", "gy", "gz")
F32 = jnp.float32
BF16 = jnp.bfloat16
FAST_GROUPS = 6
UNROLL = 3
VMEM_BYTES = 16 * 2**20
STEP = 16


def up8(count):
    return (count + 7) // 8 * 8


def level_place(level, z_bits, y_bits):
    if level < z_bits:
        return (2, level, 0 if level == 0 else -1)
    if level < z_bits + y_bits:
        return (1, level - z_bits, 1 if level == z_bits else -1)
    return (0, level - z_bits - y_bits, 2 if level == z_bits + y_bits else -1)


class Plan:
    def __init__(self, mesh, count_tiles, tile_size, levels, km, kl, kn):
        self.tiles = count_tiles
        self.size = tile_size
        self.rows = up8(count_tiles)
        self.grid = round(count_tiles ** (1 / 3))
        self.face = self.grid * self.grid
        self.levels = levels
        self.km = km
        self.kl = kl
        self.kn = kn
        self.devices = mesh.size
        z_bits = mesh.shape["gz"].bit_length() - 1
        y_bits = mesh.shape["gy"].bit_length() - 1
        x_bits = mesh.shape["gx"].bit_length() - 1
        self.place = [level_place(level, z_bits, y_bits) for level in range(levels)]
        self.near_level = [None] * 3
        for level, (_, _, slot) in enumerate(self.place):
            if slot >= 0:
                self.near_level[slot] = level
        self.frows = up8(3 * self.face)
        self.row_u = self.frows
        self.row_m = 2 * self.frows
        self.row_t = self.row_m + up8(self.face)
        self.near_rows = self.row_t + self.rows
        self.stages = []
        start = 0
        for bits in (z_bits, y_bits, x_bits):
            low = start
            while low < start + bits:
                top = min(low + 2, start + bits)
                self.stages.append(list(range(low, top)))
                low = top
            start += bits


def lane_sum(values):
    return jnp.sum(values, axis=1, keepdims=True)


def split3(values):
    high = values.astype(BF16)
    rest = values - high.astype(F32)
    middle = rest.astype(BF16)
    low = (rest - middle.astype(F32)).astype(BF16)
    return high, middle, low


def dot_nt(left, right):
    return lax.dot_general(left, right, (((1,), (1,)), ((), ())), preferred_element_type=F32)


def dot_nn(left, right):
    return lax.dot_general(left, right, (((1,), (0,)), ((), ())), preferred_element_type=F32)


PAIRS = ((0, 0), (1, 1), (2, 2), (0, 1), (0, 2), (1, 2))


def spread_sums(blocks):
    rows, size = blocks[0].shape
    tall = blocks[0] if len(blocks) == 1 else jnp.concatenate(blocks, axis=0)
    high = tall.astype(BF16)
    rest = (tall - high.astype(F32)).astype(BF16)
    sums = dot_nn(jnp.concatenate([high, rest], axis=1), jnp.ones((2 * size, size), BF16))
    return [sums[i * rows : (i + 1) * rows] for i in range(len(blocks))]


def moment_table(mass, parts):
    shape = mass.shape
    lane = lax.broadcasted_iota(jnp.int32, shape, 1)
    count = len(parts)
    total, *firsts = spread_sums([mass] + [mass * part[c] for part in parts for c in range(3)])
    columns = [(0, total)]
    rel = []
    for k, part in enumerate(parts):
        line = []
        for c in range(3):
            center = firsts[3 * k + c] / total
            columns.append((k * STEP + 1 + c, center))
            line.append(part[c] - center)
        rel.append(line)
    weighted = [[mass * line[c] for c in range(3)] for line in rel]
    terms = []
    for k in range(2 * count - 1):
        for a, b in PAIRS:
            term = None
            for i in range(count):
                j = k - i
                if 0 <= j < count:
                    item = weighted[i][a] * rel[j][b]
                    term = item if term is None else term + item
            terms.append(term)
    seconds = spread_sums(terms)
    for k in range(2 * count - 1):
        second = seconds[6 * k : 6 * k + 6]
        trace = second[0] + second[1] + second[2]
        for q in range(6):
            value = 3.0 * second[q] - trace if q < 3 else 3.0 * second[q]
            columns.append((k * STEP + 4 + q, value))
    table = jnp.zeros(shape, F32)
    for where, value in columns:
        table = jnp.where(lane == where, value, table)
    return table


def device_bits(levels):
    device = lax.axis_index(AXES)
    return [jnp.right_shift(device, level) & 1 for level in range(levels)]


def face_rows(plan, slot, bit):
    cut = 2 - slot
    grid = plan.grid
    strides = (grid * grid, grid, 1)
    others = [axis for axis in range(3) if axis != cut]
    coord = jnp.where(bit == 1, 0, grid - 1)
    base = coord * strides[cut]
    return [
        base + s // grid * strides[others[0]] + s % grid * strides[others[1]]
        for s in range(plan.face)
    ]


def first_kernel(plan, *refs):
    ins, (base_ref, mom_ref, id_ref), near_refs = refs[:5], refs[5:8], refs[8:11]
    buffers, sems = refs[11:16], refs[16]
    copies = [pltpu.make_async_copy(ins[i], buffers[i], sems.at[i]) for i in range(5)]
    for copy in copies:
        copy.start()
    for copy in copies:
        copy.wait()
    off_ref, vel_ref, mass_ref, act_ref, far_ref = buffers
    tiles, rows, size, grid = plan.tiles, plan.rows, plan.size, plan.grid
    tile = lax.broadcasted_iota(jnp.int32, (rows, size), 0)
    base_ref[...] = jnp.zeros(base_ref.shape, F32)
    for t in range(tiles):
        lanes = pl.ds(t * size, size)
        for c in range(3):
            base_ref[c, pl.ds(t, 1), :] = off_ref[pl.ds(c, 1), lanes]
            base_ref[4 + c, pl.ds(t, 1), :] = vel_ref[pl.ds(c, 1), lanes]
    base_ref[3, pl.ds(0, tiles), :] = mass_ref[...]
    base_ref[7, pl.ds(0, tiles), :] = act_ref[...].astype(F32)
    corners = (tile // (grid * grid), tile // grid % grid, tile % grid)
    inside = tile < tiles
    act = base_ref[7]
    position = []
    for c in range(3):
        value = jnp.where(inside, base_ref[c] + corners[c].astype(F32), 0.0)
        base_ref[c] = value
        position.append(value)
    mass = jnp.where(inside, base_ref[3], 1.0)
    base_ref[3] = mass
    table = moment_table(mass, [position])
    mom_ref[...] = table
    lists = plan.levels * plan.km
    flat = jnp.concatenate(
        [far_ref[level].astype(F32) for level in range(plan.levels)]
        + [jnp.zeros((up8(lists) - lists, tiles), F32)] * (lists % 8 > 0),
        axis=0,
    )
    id_ref[pl.ds(0, tiles), pl.ds(0, up8(lists))] = jnp.transpose(flat).astype(jnp.int32)
    bits = device_bits(plan.levels)
    for slot, ref in enumerate(near_refs):
        ref[pl.ds(plan.row_t, rows), :] = table
        for s, row in enumerate(face_rows(plan, slot, bits[plan.near_level[slot]])):
            for c in range(3):
                ref[pl.ds(c * plan.face + s, 1), :] = base_ref[c, pl.ds(row, 1), :]
                ref[pl.ds(plan.row_u + c * plan.face + s, 1), :] = (
                    base_ref[4 + c, pl.ds(row, 1), :] * base_ref[7, pl.ds(row, 1), :]
                )
            ref[pl.ds(plan.row_m + s, 1), :] = base_ref[3, pl.ds(row, 1), :]


def far_picks(plan, far_ref, pick_ref):
    rows, size = plan.rows, plan.size
    lane = lax.broadcasted_iota(jnp.int32, (rows, size), 1)
    ids = far_ref[...].astype(F32)
    items = plan.levels * plan.km
    tall = jnp.concatenate([jnp.where(lane == i, ids, 0.0) for i in range(items)], axis=0)
    spread = dot_nn(tall.astype(BF16), jnp.ones((size, size), BF16))
    cell = jnp.where(lane < 3 * rows, lane % rows, -1).astype(F32)
    for i in range(items):
        hit = spread[i * rows : (i + 1) * rows] == cell
        pick_ref[i] = jnp.where(hit, 1.0, 0.0).astype(BF16)


def far_field(plan, pick_ref, tables, target):
    rows, size = plan.rows, plan.size
    total = [jnp.zeros((rows, size), F32) for _ in range(3)]
    one = jnp.where(
        lax.broadcasted_iota(jnp.int32, (16, size), 0)
        == lax.broadcasted_iota(jnp.int32, (16, size), 1),
        1.0,
        0.0,
    ).astype(BF16)
    half = lax.broadcasted_iota(jnp.int32, (2 * size, 2 * size), 0) < size
    left = lax.broadcasted_iota(jnp.int32, (2 * size, 2 * size), 1) < size
    ones = jnp.where(half == left, 1.0, 0.0).astype(BF16)
    blank = jnp.zeros((size - 3 * rows, size), BF16)
    for level in range(plan.levels):
        flat = dot_nt(one, jnp.concatenate([*split3(tables[level]), blank], axis=0)).astype(BF16)
        wide = [jnp.broadcast_to(flat[p : p + 1], (rows, size)) for p in range(10)]
        picks = [pick_ref[level * plan.km + k] for k in range(plan.km)]
        tall = [
            jnp.concatenate([pick * wide[p], pick * wide[p + 5]], axis=1)
            for pick in picks
            for p in range(5)
        ]
        got = dot_nn(jnp.concatenate(tall, axis=0), ones)
        for k in range(plan.km):
            own = [got[(5 * k + p) * rows : (5 * k + p + 1) * rows] for p in range(5)]
            q = [part[:, :size] for part in own] + [part[:, size:] for part in own]
            r = [target[c] - q[1 + c] for c in range(3)]
            inverse = lax.rsqrt(r[0] * r[0] + r[1] * r[1] + r[2] * r[2] + SOFT2)
            inverse_sq = inverse * inverse
            cube = inverse * inverse_sq
            fifth = cube * inverse_sq
            dot = [
                q[4] * r[0] + q[7] * r[1] + q[8] * r[2],
                q[7] * r[0] + q[5] * r[1] + q[9] * r[2],
                q[8] * r[0] + q[9] * r[1] + q[6] * r[2],
            ]
            form = r[0] * dot[0] + r[1] * dot[1] + r[2] * dot[2]
            scale = q[0] * cube + 2.5 * form * (fifth * inverse_sq)
            for c in range(3):
                total[c] = total[c] + (dot[c] * fifth - scale * r[c])
    return total


class Near:
    def __init__(self, plan, rank_ref, src_ref, lists, face_ref=None):
        self.plan = plan
        self.rank_ref = rank_ref
        self.src_ref = src_ref
        self.lists = lists
        self.face_ref = face_ref

    def one_hot(self, t, first, count):
        slot = lax.broadcasted_iota(jnp.int32, (count, self.plan.size), 0).astype(F32)
        return self.rank_ref[pl.ds(t, 1), :] == slot + first

    def compact(self, t, first, count, values):
        size = self.plan.size
        pick = jnp.where(self.one_hot(t, first, count), 1.0, 0.0).astype(BF16)
        sub = lax.broadcasted_iota(jnp.int32, (8, size), 0)
        own = jnp.broadcast_to(values[-1], (8, size))
        for i in range(len(values) - 2, -1, -1):
            own = jnp.where(sub == i, values[i], own)
        high, middle, low = split3(own)
        return dot_nt(pick, high) + dot_nt(pick, middle) + dot_nt(pick, low)

    def local_rows(self, t):
        found = []
        for s in range(self.plan.kl):
            index = self.lists[0][s, t]
            found.append([self.src_ref[c, pl.ds(index, 1), :] for c in range(4)])
        return found

    def remote_rows(self, t):
        found = []
        for slot in range(3):
            for k in range(self.plan.kn):
                index = self.lists[1][slot, k, t]
                found.append([self.face_ref[slot, c, pl.ds(index, 1), :] for c in range(4)])
        return found

    def pair_sums(self, here, sources, sums=None):
        for source in sources:
            r = [source[c] - here[c] for c in range(3)]
            inverse = lax.rsqrt(r[0] * r[0] + r[1] * r[1] + r[2] * r[2] + SOFT2)
            strength = source[3] * inverse * (inverse * inverse)
            new = [r[c] * strength for c in range(3)]
            sums = new if sums is None else [sums[c] + new[c] for c in range(3)]
        return sums

    def spread(self, packed):
        return [jnp.broadcast_to(packed[:, c : c + 1], (8, self.plan.size)) for c in range(3)]

    def prepare(self, t, comp_ref, wide_ref):
        shape = (FAST_GROUPS * 8, self.plan.size)
        for c in range(3):
            value = jnp.broadcast_to(comp_ref[t, :, pl.ds(c, 1)], shape)
            for g in range(FAST_GROUPS):
                wide_ref[t, g, c] = value[g * 8 : g * 8 + 8]

    def force(self, t, rows, wide_ref, part_ref, init_ref=None):
        for g in range(FAST_GROUPS):
            here = [wide_ref[t, g, c] for c in range(3)]
            sums = None if init_ref is None else [init_ref[t, g, c] for c in range(3)]
            for c, value in enumerate(self.pair_sums(here, rows, sums)):
                part_ref[t, g, c] = value

    def scatter(self, t, part_ref, row_ref):
        out = [None] * 3
        for g in range(FAST_GROUPS):
            mask = self.one_hot(t, g * 8, 8)
            for c in range(3):
                value = jnp.where(mask, lane_sum(part_ref[t, g, c]), 0.0)
                out[c] = value if out[c] is None else out[c] + value
        for c in range(3):
            row_ref[c, pl.ds(t, 1), :] = jnp.sum(out[c], axis=0, keepdims=True)

    def rest(self, row_ref):
        @pl.when(jnp.max(self.rank_ref[...]) >= FAST_GROUPS * 8)
        def _():
            def tile_rest(t, carry):
                def group(g, inner):
                    values = [self.src_ref[c, pl.ds(t, 1), :] for c in range(3)]
                    here = self.spread(self.compact(t, g * 8, 8, values))
                    sums = self.pair_sums(here, self.local_rows(t) + self.remote_rows(t))
                    mask = self.one_hot(t, g * 8, 8)
                    for c in range(3):
                        value = jnp.where(mask, lane_sum(sums[c]), 0.0)
                        old = row_ref[c, pl.ds(t, 1), :]
                        row_ref[c, pl.ds(t, 1), :] = old + jnp.sum(value, axis=0, keepdims=True)
                    return inner

                most = jnp.max(self.rank_ref[pl.ds(t, 1), :]).astype(jnp.int32)
                lax.fori_loop(FAST_GROUPS, (most + 8) // 8, group, 0)
                return carry

            lax.fori_loop(0, self.plan.tiles, tile_rest, 0)


def shift_of(plan, level, bit):
    _, place, _ = plan.place[level]
    span = float(plan.grid * 2**place)
    return jnp.where(bit == 0, span, -span).astype(F32)


def lists_start(ins, outs, sems):
    copies = [pltpu.make_async_copy(ins[i], outs[i], sems.at[i]) for i in range(2)]
    for copy in copies:
        copy.start()

    def arrived():
        for copy in copies:
            copy.wait()
        return outs

    return arrived


def rank_rows(plan, act):
    size = plan.size
    below = lax.broadcasted_iota(jnp.int32, (size, size), 0) < lax.broadcasted_iota(
        jnp.int32, (size, size), 1
    )
    rank = dot_nn(act.astype(BF16), jnp.where(below, 1.0, 0.0).astype(BF16))
    return jnp.where(act > 0, rank, -1.0)


def tile_loop(plan, step):
    def body(i, carry):
        step([jnp.minimum(i * UNROLL + j, plan.tiles - 1) for j in range(UNROLL)])
        return carry

    lax.fori_loop(0, (plan.tiles + UNROLL - 1) // UNROLL, body, 0)


def local_kernel(plan, *refs):
    arrived = lists_start(refs[:2], refs[-3:-1], refs[-1])
    base_ref, far_ref, rank_ref, pick_ref, comp_ref, wide_ref, part_ref = refs[2:9]
    tiles = plan.tiles
    rank_ref[...] = rank_rows(plan, base_ref[7])
    far_picks(plan, far_ref, pick_ref)
    near = Near(plan, rank_ref, base_ref, None)
    for t in range(tiles):
        own = base_ref[7, pl.ds(t, 1), :]
        values = [base_ref[c, pl.ds(t, 1), :] for c in range(3)]
        values += [base_ref[4 + c, pl.ds(t, 1), :] * own for c in range(3)]
        comp_ref[t, :, pl.ds(0, 8)] = near.compact(t, 0, FAST_GROUPS * 8, values)
    for j in range(UNROLL):
        near.prepare(min(j, tiles - 1), comp_ref, wide_ref)
    near.lists = arrived()

    def step(ts):
        for t in ts:
            near.force(t, near.local_rows(t), wide_ref, part_ref)
        for t in ts:
            near.prepare(jnp.minimum(t + UNROLL, tiles - 1), comp_ref, wide_ref)

    tile_loop(plan, step)


def gather_kernel(plan, rank_ref, comp_ref, acc_ref, u_ref, a_ref):
    near = Near(plan, rank_ref, acc_ref, None)
    for t in range(plan.tiles):
        values = [acc_ref[c, pl.ds(t, 1), :] for c in range(3)]
        a_ref[t, :, pl.ds(0, 8)] = near.compact(t, 0, FAST_GROUPS * 8, values)
        u_ref[t] = pltpu.roll(comp_ref[t], plan.size - 3, 1)


def lane_row(plan, level, bit):
    cut, _, _ = plan.place[level]
    lane = lax.broadcasted_iota(jnp.int32, (1, plan.size), 1)
    return jnp.where(lane == 1 + cut, shift_of(plan, level, bit), 0.0)


def square_row(acc):
    square = acc[0] * acc[0] + acc[1] * acc[1] + acc[2] * acc[2]
    return jnp.max(square, axis=0, keepdims=True)


def time_step_of(square):
    return ETA / jnp.sqrt(jnp.sqrt(square) + 1e-06)


def second_kernel(plan, *refs):
    face_ref, part_ref, row_ref, *smem = refs[-6:]
    arrived, refs = lists_start(refs[:2], smem[:2], smem[2]), refs[2:]
    base_ref, pick_ref, rank_ref, wide_ref, init_ref = refs[:5]
    near_refs = refs[5:8]
    extra = plan.levels - 3
    moment_refs = refs[8 : 8 + extra]
    acc_ref, max_ref, mom_ref = refs[8 + extra : 11 + extra]
    send_refs = refs[11 + extra : 14 + extra]
    rows, tiles = plan.rows, plan.tiles
    bits = device_bits(plan.levels)
    face = plan.face
    for slot in range(3):
        level = plan.near_level[slot]
        cut = plan.place[level][0]
        for c in range(3):
            value = near_refs[slot][pl.ds(c * face, face), :]
            if c == cut:
                value = value + shift_of(plan, level, bits[level])
            face_ref[slot, c, pl.ds(0, face), :] = value
        face_ref[slot, 3, pl.ds(0, face), :] = near_refs[slot][pl.ds(plan.row_m, face), :]
    tables = []
    others = list(moment_refs)
    for level in range(plan.levels):
        slot = plan.place[level][2]
        table = near_refs[slot][pl.ds(plan.row_t, rows), :] if slot >= 0 else others.pop(0)[...]
        tables.append(table + lane_row(plan, level, bits[level]))
    act = base_ref[7]
    position = [base_ref[c] for c in range(3)]
    far = far_field(plan, pick_ref, tables, position)
    row_ref[...] = jnp.zeros(row_ref.shape, F32)
    near = Near(plan, rank_ref, base_ref, arrived(), face_ref)

    def step(ts):
        for t in ts:
            near.scatter(jnp.maximum(t - UNROLL, 0), part_ref, row_ref)
        for t in ts:
            near.force(t, near.remote_rows(t), wide_ref, part_ref, init_ref)

    tile_loop(plan, step)
    for j in range(UNROLL):
        near.scatter(max(tiles - 1 - j, 0), part_ref, row_ref)
    near.rest(row_ref)
    acc = [act * (GRAV * (row_ref[c] + far[c])) for c in range(3)]
    for c in range(3):
        acc_ref[c] = acc[c]
    max_ref[...] = square_row(acc)
    table = moment_table(base_ref[3], [position, [base_ref[4 + c] * act for c in range(3)], acc])
    mom_ref[...] = table
    for slot, ref in enumerate(send_refs):
        ref[pl.ds(plan.frows, rows), :] = table
        for s, row in enumerate(face_rows(plan, slot, bits[plan.near_level[slot]])):
            for c in range(3):
                ref[pl.ds(c * face + s, 1), :] = acc_ref[c, pl.ds(row, 1), :]


def third_kernel(plan, *refs):
    face_ref, part_ref, row_ref, src_ref, moved_ref, slot_ref, wide_ref, *smem = refs[-10:]
    arrived, refs = lists_start(refs[:2], smem[:2], smem[2]), refs[2:]
    base_ref, pick_ref, rank_ref, comp_ref, u_ref, a_ref, acc_ref, max_ref = refs[:8]
    near_refs = refs[8:11]
    send_refs = refs[11:14]
    extra = plan.levels - 3
    moment_refs = refs[14 : 14 + extra]
    pos_ref, out_ref, square_ref, step_ref = refs[14 + extra : 18 + extra]
    rows, size, tiles = plan.rows, plan.size, plan.tiles
    bits = device_bits(plan.levels)
    step = time_step_of(jnp.max(max_ref[...], axis=(0, 1), keepdims=True))
    step_ref[...] = jnp.broadcast_to(step, step_ref.shape)
    wide = jnp.broadcast_to(step, (rows, size))
    position = []
    act = base_ref[7]
    for c in range(3):
        moved = base_ref[c] + (base_ref[4 + c] * act + acc_ref[c] * wide) * wide
        pos_ref[c] = moved
        src_ref[c] = moved
        position.append(moved)
    src_ref[3] = base_ref[3]
    slots = jnp.broadcast_to(step, (FAST_GROUPS * 8, size))
    for t in range(tiles):
        slot_ref[t] = comp_ref[t] + (u_ref[t] + a_ref[t] * slots) * slots
    lane = lax.broadcasted_iota(jnp.int32, (rows, size), 1)
    tables = []
    others = list(moment_refs)
    for level in range(plan.levels):
        slot = plan.place[level][2]
        table = send_refs[slot][pl.ds(plan.frows, rows), :] if slot >= 0 else others.pop(0)[...]
        total = None
        for k in range(4, -1, -1):
            part = pltpu.roll(table, size - k * STEP, 1) if k else table
            total = part if total is None else total * wide + part
        tables.append(jnp.where(lane < 10, total, 0.0) + lane_row(plan, level, bits[level]))
    face = plan.face
    frows = plan.frows
    fwide = jnp.broadcast_to(step, (frows, size))
    for slot in range(3):
        level = plan.near_level[slot]
        cut = plan.place[level][0]
        got = near_refs[slot]
        moved_ref[slot] = (
            got[pl.ds(0, frows), :]
            + (got[pl.ds(plan.row_u, frows), :] + send_refs[slot][pl.ds(0, frows), :] * fwide)
            * fwide
        )
        for c in range(3):
            value = moved_ref[slot, pl.ds(c * face, face), :]
            if c == cut:
                value = value + shift_of(plan, level, bits[level])
            face_ref[slot, c, pl.ds(0, face), :] = value
        face_ref[slot, 3, pl.ds(0, face), :] = got[pl.ds(plan.row_m, face), :]
    far = far_field(plan, pick_ref, tables, position)
    row_ref[...] = jnp.zeros(row_ref.shape, F32)
    near = Near(plan, rank_ref, src_ref, arrived(), face_ref)
    for j in range(UNROLL):
        near.prepare(min(j, tiles - 1), slot_ref, wide_ref)

    def work(ts):
        for t in ts:
            near.scatter(jnp.maximum(t - UNROLL, 0), part_ref, row_ref)
        for t in ts:
            near.force(t, near.local_rows(t) + near.remote_rows(t), wide_ref, part_ref)
        for t in ts:
            near.prepare(jnp.minimum(t + UNROLL, tiles - 1), slot_ref, wide_ref)

    tile_loop(plan, work)
    for j in range(UNROLL):
        near.scatter(max(tiles - 1 - j, 0), part_ref, row_ref)
    near.rest(row_ref)
    acc = [act * (GRAV * (row_ref[c] + far[c])) for c in range(3)]
    for c in range(3):
        out_ref[c] = acc[c]
    square_ref[...] = square_row(acc)


def last_kernel(plan, max_ref, base_ref, pos_ref, first_ref, acc_ref, step_ref,
                pos_out, vel_out, acc_out, steps_out, work_ref):
    rows, size = plan.rows, plan.size
    second = time_step_of(jnp.max(max_ref[...], axis=(0, 1), keepdims=True))
    one = step_ref[...]
    steps_out[0] = one[0, 0]
    steps_out[1] = second[0, 0]
    first = jnp.broadcast_to(one[:, :1], (rows, size))
    wide = jnp.broadcast_to(second, (rows, size))
    act = base_ref[7]
    for c in range(3):
        velocity = base_ref[4 + c] + first_ref[c] * first + acc_ref[c] * wide
        work_ref[0, c] = pos_ref[c] + velocity * act * wide
        work_ref[1, c] = velocity
    for t in range(plan.tiles):
        lanes = pl.ds(t * size, size)
        for c in range(3):
            pos_out[pl.ds(c, 1), lanes] = work_ref[0, c, pl.ds(t, 1), :]
            vel_out[pl.ds(c, 1), lanes] = work_ref[1, c, pl.ds(t, 1), :]
            acc_out[pl.ds(c, 1), lanes] = acc_ref[c, pl.ds(t, 1), :]


def vmem():
    return pl.BlockSpec(memory_space=pltpu.VMEM)


def hbm():
    return pl.BlockSpec(memory_space=pltpu.HBM)


def in_hbm(values):
    return pltpu.with_memory_space_constraint(values, pltpu.HBM)


def smem():
    return pl.BlockSpec(memory_space=pltpu.SMEM)


def call(kernel, outs, scratch, specs, name, out_specs=None):
    return pl.pallas_call(
        kernel,
        out_shape=outs,
        in_specs=specs,
        out_specs=out_specs or [vmem() for _ in outs],
        scratch_shapes=scratch,
        compiler_params=pltpu.CompilerParams(vmem_limit_bytes=VMEM_BYTES),
        name=name,
    )


def buffers(*shapes):
    return [pltpu.VMEM(shape, F32) for shape in shapes]


def floats(*shapes):
    return [jax.ShapeDtypeStruct(shape, F32) for shape in shapes]


def exchange(plan, block, bits):
    flip = sum(1 << bit for bit in bits)
    return lax.ppermute(block, AXES, [(i, i ^ flip) for i in range(plan.devices)])


def body(mesh, offsets, velocities, masses, active, near_local, near_remote, far_list):
    tiles, kl = near_local.shape
    kn = near_remote.shape[2]
    levels, km = far_list.shape[1:]
    size = masses.shape[0] // tiles
    plan = Plan(mesh, tiles, size, levels, km, kl, kn)
    rows, near_rows = plan.rows, plan.near_rows
    whole = (3, rows, size)
    extra = levels - 3
    base, moments, far_ids, *near = call(
        functools.partial(first_kernel, plan),
        floats((8, rows, size), (rows, size))
        + [jax.ShapeDtypeStruct((rows, size), jnp.int32)]
        + floats(*[(near_rows, size)] * 3),
        buffers(offsets.shape, velocities.shape, (tiles, size))
        + [
            pltpu.VMEM((tiles, size), jnp.int32),
            pltpu.VMEM((levels, km, tiles), jnp.int32),
            pltpu.SemaphoreType.DMA((5,)),
        ],
        [hbm()] * 5,
        "first",
    )(
        in_hbm(offsets),
        in_hbm(velocities),
        in_hbm(masses.reshape(tiles, size)),
        in_hbm(active.reshape(tiles, size)),
        in_hbm(jnp.transpose(far_list, (1, 2, 0))),
    )

    got_near = [None] * 3
    got_far = []
    for slot in range(3):
        got_near[slot] = exchange(plan, near[slot], [plan.near_level[slot]])
    for level in range(levels):
        if plan.place[level][2] < 0:
            got_far.append(exchange(plan, moments, [level]))

    lists = (
        in_hbm(jnp.transpose(near_local)),
        in_hbm(jnp.transpose(near_remote, (1, 2, 0))),
    )
    slots = (tiles, FAST_GROUPS * 8, size)
    broad = (tiles, FAST_GROUPS, 3, 8, size)
    list_scratch = [
        pltpu.SMEM((kl, tiles), jnp.int32),
        pltpu.SMEM((3, kn, tiles), jnp.int32),
        pltpu.SemaphoreType.DMA((2,)),
    ]
    force_scratch = buffers((3, 4, up8(plan.face), size), broad, whole)
    rank, picks, comp, spread, local = call(
        functools.partial(local_kernel, plan),
        floats((rows, size))
        + [jax.ShapeDtypeStruct((levels * km, rows, size), BF16)]
        + floats(slots, broad, broad),
        list_scratch,
        [hbm(), hbm(), vmem(), vmem()],
        "local",
    )(*lists, base, far_ids)
    send_rows = plan.frows + rows
    acc, square, table, *send = call(
        functools.partial(second_kernel, plan),
        floats(whole, (1, size), (rows, size), *[(send_rows, size)] * 3),
        force_scratch + list_scratch,
        [hbm(), hbm()] + [vmem()] * (5 + levels),
        "second",
    )(*lists, base, picks, rank, spread, local, *got_near, *got_far)
    slot_u, slot_a = call(
        functools.partial(gather_kernel, plan),
        floats(slots, slots),
        [],
        [vmem()] * 3,
        "gather",
    )(rank, comp, acc)

    got_send = [None] * 3
    got_table = {}
    best = square
    for stage in plan.stages:
        flips = [[bit] for bit in stage] + ([stage] if len(stage) > 1 else [])
        seen = [best]
        for flip in flips:
            slot = plan.place[flip[0]][2] if len(flip) == 1 else -1
            if len(flip) > 1:
                seen.append(exchange(plan, best, flip))
                continue
            data = send[slot] if slot >= 0 else table
            there = exchange(plan, jnp.concatenate([data, best], axis=0), flip)
            seen.append(there[data.shape[0] :])
            if slot >= 0:
                got_send[slot] = there
            else:
                got_table[flip[0]] = there
        best = functools.reduce(jnp.maximum, seen)
    moved, acc2, square2, step = call(
        functools.partial(third_kernel, plan),
        floats(whole, whole, (1, size), (1, size)),
        force_scratch
        + buffers((4, rows, size), (3, plan.frows, size), slots, broad)
        + list_scratch,
        [hbm(), hbm()] + [vmem()] * (8 + 3 + 3 + extra),
        "third",
    )(
        *lists, base, picks, rank, comp, slot_u, slot_a, acc, best, *got_near, *got_send,
        *[got_table[level][:rows] for level in range(levels) if plan.place[level][2] < 0],
    )
    copies = jnp.broadcast_to(square2[None], (plan.devices, 1, size))
    everyone = lax.all_to_all(copies, AXES, 0, 0).reshape(plan.devices, size)
    pos, vel, out, steps = call(
        functools.partial(last_kernel, plan),
        floats(offsets.shape, offsets.shape, offsets.shape, (SUBSTEPS,)),
        buffers((2, 3, rows, size)),
        [vmem()] * 6,
        "last",
        [vmem(), vmem(), vmem(), smem()],
    )(everyone, base, moved, acc, acc2, step)
    return pos, vel, out, steps


def solution(mesh):
    parts = P(None, AXES)
    return jax.shard_map(
        functools.partial(body, mesh),
        mesh=mesh,
        in_specs=(parts, parts, P(AXES), P(AXES), P(AXES, None), P(AXES, None, None), P(AXES, None, None)),
        out_specs=(parts, parts, parts, P()),
        check_vma=False,
    )
```

```python
import functools

import jax
import jax.numpy as jnp
from jax import lax
from jax.experimental import pallas as pl
from jax.experimental.pallas import tpu as pltpu
from jax.sharding import PartitionSpec as P

SUBSTEPS = 2
GRAV = 0.02
SOFT2 = 0.0025
ETA = 0.15
AXES = ("gx", "gy", "gz")
F32 = jnp.float32
BF16 = jnp.bfloat16
FAST_GROUPS = 6
UNROLL = 3
VMEM_BYTES = 16 * 2**20
FOLD = 16


def up8(count):
    return (count + 7) // 8 * 8


def level_place(level, z_bits, y_bits):
    if level < z_bits:
        return (2, level, 0 if level == 0 else -1)
    if level < z_bits + y_bits:
        return (1, level - z_bits, 1 if level == z_bits else -1)
    return (0, level - z_bits - y_bits, 2 if level == z_bits + y_bits else -1)


class Plan:
    def __init__(self, mesh, count_tiles, tile_size, levels, km, kl, kn):
        self.tiles = count_tiles
        self.size = tile_size
        self.rows = up8(count_tiles)
        self.grid = round(count_tiles ** (1 / 3))
        self.face = self.grid * self.grid
        self.levels = levels
        self.km = km
        self.kl = kl
        self.kn = kn
        self.devices = mesh.size
        z_bits = mesh.shape["gz"].bit_length() - 1
        y_bits = mesh.shape["gy"].bit_length() - 1
        self.place = [level_place(level, z_bits, y_bits) for level in range(levels)]
        self.near_level = [None] * 3
        for level, (_, _, slot) in enumerate(self.place):
            if slot >= 0:
                self.near_level[slot] = level
        self.frows = up8(3 * self.face)
        self.row_u = self.frows
        self.row_m = 2 * self.frows
        self.row_t = self.row_m + up8(self.face)
        self.near_rows = self.row_t + self.rows


def lane_sum(values):
    return jnp.sum(values, axis=1, keepdims=True)


def split3(values):
    high = values.astype(BF16)
    rest = values - high.astype(F32)
    middle = rest.astype(BF16)
    low = (rest - middle.astype(F32)).astype(BF16)
    return high, middle, low


def dot_nt(left, right):
    return lax.dot_general(left, right, (((1,), (1,)), ((), ())), preferred_element_type=F32)


def dot_nn(left, right):
    return lax.dot_general(left, right, (((1,), (0,)), ((), ())), preferred_element_type=F32)


PAIRS = ((0, 0), (1, 1), (2, 2), (0, 1), (0, 2), (1, 2))


def spread_sums(blocks):
    rows, size = blocks[0].shape
    tall = blocks[0] if len(blocks) == 1 else jnp.concatenate(blocks, axis=0)
    high = tall.astype(BF16)
    rest = (tall - high.astype(F32)).astype(BF16)
    sums = dot_nn(jnp.concatenate([high, rest], axis=1), jnp.ones((2 * size, size), BF16))
    return [sums[i * rows : (i + 1) * rows] for i in range(len(blocks))]


def lane_of(k, p):
    if k == 0:
        return p
    return 8 * (k - 1) + p - 4 if p > 3 else (6, 7, 14, 15, 22, 23)[3 * (k - 1) + p - 1]


def moment_table(mass, parts, low):
    shape = mass.shape
    lane = lax.broadcasted_iota(jnp.int32, shape, 1)
    count = len(parts)
    total, *firsts = spread_sums([mass] + [mass * part[c] for part in parts for c in range(3)])
    columns = [(0, 0, total)]
    rel = []
    for k, part in enumerate(parts):
        line = []
        for c in range(3):
            center = firsts[3 * k + c] / total
            columns.append((k, 1 + c, center))
            line.append(part[c] - center)
        rel.append(line)
    weighted = [[mass * line[c] for c in range(3)] for line in rel]
    terms = []
    for k in range(2 * count - 1):
        for a, b in PAIRS:
            term = None
            for i in range(count):
                j = k - i
                if 0 <= j < count:
                    item = weighted[i][a] * rel[j][b]
                    term = item if term is None else term + item
            terms.append(term)
    seconds = spread_sums(terms)
    for k in range(2 * count - 1):
        second = seconds[6 * k : 6 * k + 6]
        trace = second[0] + second[1] + second[2]
        for q in range(6):
            value = 3.0 * second[q] - trace if q < 3 else 3.0 * second[q]
            columns.append((k, 4 + q, value))
    table = jnp.zeros(shape, F32)
    for k, p, value in columns:
        if low <= k and (k > 0 or low == 0):
            table = jnp.where(lane == lane_of(k, p), value, table)
    return table


def fold_matrix(size, steps):
    row = lax.broadcasted_iota(jnp.int32, (16, size), 0)
    lane = lax.broadcasted_iota(jnp.int32, (16, size), 1)
    hit = (row == lane) & (row < 10)
    if steps:
        for k in range(1, 5):
            for p in range(1, 10):
                if p > 3 or k < 3:
                    hit = hit | ((row == p) & (lane == FOLD + lane_of(k, p)))
    return jnp.where(hit, 1.0, 0.0).astype(BF16)


def powers_row(step, size):
    lane = lax.broadcasted_iota(jnp.int32, (1, size), 1)
    out = jnp.zeros((1, size), F32)
    power = step
    for k in range(1, 5):
        hit = None
        for p in range(1, 10):
            if p > 3 or k < 3:
                one = lane == FOLD + lane_of(k, p)
                hit = one if hit is None else hit | one
        out = jnp.where(hit, power, out)
        power = power * step
    return out


def pack_table(table, square):
    rows, size = table.shape
    blocks = rows // 8
    width = size // blocks
    row = lax.broadcasted_iota(jnp.int32, (8, size), 0)
    lane = lax.broadcasted_iota(jnp.int32, (8, size), 1)
    out = table[:8]
    for j in range(1, blocks):
        out = jnp.where(lane < j * width, out, pltpu.roll(table[8 * j : 8 * j + 8], j * width, 1))
    return jnp.where((row == 7) & (lane >= size - width), square, out)


def unpack_table(packed, rows):
    size = packed.shape[1]
    blocks = rows // 8
    width = size // blocks
    return jnp.concatenate(
        [pltpu.roll(packed, (FOLD - j * width) % size, 1) for j in range(blocks)], axis=0
    )


def device_bits(levels):
    device = lax.axis_index(AXES)
    return [jnp.right_shift(device, level) & 1 for level in range(levels)]


def face_rows(plan, slot, bit):
    cut = 2 - slot
    grid = plan.grid
    strides = (grid * grid, grid, 1)
    others = [axis for axis in range(3) if axis != cut]
    coord = jnp.where(bit == 1, 0, grid - 1)
    base = coord * strides[cut]
    return [
        base + s // grid * strides[others[0]] + s % grid * strides[others[1]]
        for s in range(plan.face)
    ]


def first_kernel(plan, *refs):
    ins, (base_ref, mom_ref, id_ref), near_refs = refs[:5], refs[5:8], refs[8:11]
    buffers, sems = refs[11:16], refs[16]
    copies = [pltpu.make_async_copy(ins[i], buffers[i], sems.at[i]) for i in range(5)]
    for copy in copies:
        copy.start()
    for copy in copies:
        copy.wait()
    off_ref, vel_ref, mass_ref, act_ref, far_ref = buffers
    tiles, rows, size, grid = plan.tiles, plan.rows, plan.size, plan.grid
    tile = lax.broadcasted_iota(jnp.int32, (rows, size), 0)
    base_ref[...] = jnp.zeros(base_ref.shape, F32)
    for t in range(tiles):
        lanes = pl.ds(t * size, size)
        for c in range(3):
            base_ref[c, pl.ds(t, 1), :] = off_ref[pl.ds(c, 1), lanes]
            base_ref[4 + c, pl.ds(t, 1), :] = vel_ref[pl.ds(c, 1), lanes]
    base_ref[3, pl.ds(0, tiles), :] = mass_ref[...]
    base_ref[7, pl.ds(0, tiles), :] = act_ref[...].astype(F32)
    corners = (tile // (grid * grid), tile // grid % grid, tile % grid)
    inside = tile < tiles
    act = base_ref[7]
    position = []
    for c in range(3):
        value = jnp.where(inside, base_ref[c] + corners[c].astype(F32), 0.0)
        base_ref[c] = value
        position.append(value)
    mass = jnp.where(inside, base_ref[3], 1.0)
    base_ref[3] = mass
    table = moment_table(mass, [position], 0)
    mom_ref[...] = table
    lists = plan.levels * plan.km
    flat = jnp.concatenate(
        [far_ref[level].astype(F32) for level in range(plan.levels)]
        + [jnp.zeros((up8(lists) - lists, tiles), F32)] * (lists % 8 > 0),
        axis=0,
    )
    id_ref[pl.ds(0, tiles), pl.ds(0, up8(lists))] = jnp.transpose(flat).astype(jnp.int32)
    bits = device_bits(plan.levels)
    for slot, ref in enumerate(near_refs):
        ref[pl.ds(plan.row_t, rows), :] = table
        for s, row in enumerate(face_rows(plan, slot, bits[plan.near_level[slot]])):
            for c in range(3):
                ref[pl.ds(c * plan.face + s, 1), :] = base_ref[c, pl.ds(row, 1), :]
                ref[pl.ds(plan.row_u + c * plan.face + s, 1), :] = (
                    base_ref[4 + c, pl.ds(row, 1), :] * base_ref[7, pl.ds(row, 1), :]
                )
            ref[pl.ds(plan.row_m + s, 1), :] = base_ref[3, pl.ds(row, 1), :]


def far_picks(plan, far_ref, pick_ref):
    rows, size = plan.rows, plan.size
    lane = lax.broadcasted_iota(jnp.int32, (rows, size), 1)
    ids = far_ref[...].astype(F32)
    items = plan.levels * plan.km
    tall = jnp.concatenate([jnp.where(lane == i, ids, 0.0) for i in range(items)], axis=0)
    spread = dot_nn(tall.astype(BF16), jnp.ones((size, size), BF16))
    cell = jnp.where(lane < 3 * rows, lane % rows, -1).astype(F32)
    for i in range(items):
        hit = spread[i * rows : (i + 1) * rows] == cell
        pick_ref[i] = jnp.where(hit, 1.0, 0.0).astype(BF16)


def far_field(plan, pick_ref, tables, fold, target):
    rows, size = plan.rows, plan.size
    total = [jnp.zeros((rows, size), F32) for _ in range(3)]
    half = lax.broadcasted_iota(jnp.int32, (2 * size, 2 * size), 0) < size
    left = lax.broadcasted_iota(jnp.int32, (2 * size, 2 * size), 1) < size
    ones = jnp.where(half == left, 1.0, 0.0).astype(BF16)
    lane = lax.broadcasted_iota(jnp.int32, (16, size), 1)
    blank = jnp.zeros((size - 3 * rows, size), BF16)
    for level in range(plan.levels):
        parts = [dot_nt(fold, jnp.concatenate([x, x, x, blank], axis=0)) for x in split3(tables[level])]
        high, middle, low = split3(parts[0] + parts[1] + parts[2])
        flat = jnp.where(
            lane < rows,
            high.astype(F32),
            jnp.where(lane < 2 * rows, middle.astype(F32), low.astype(F32)),
        ).astype(BF16)
        wide = [jnp.broadcast_to(flat[p : p + 1], (rows, size)) for p in range(10)]
        picks = [pick_ref[level * plan.km + k] for k in range(plan.km)]
        tall = [
            jnp.concatenate([pick * wide[p], pick * wide[p + 5]], axis=1)
            for pick in picks
            for p in range(5)
        ]
        got = dot_nn(jnp.concatenate(tall, axis=0), ones)
        for k in range(plan.km):
            own = [got[(5 * k + p) * rows : (5 * k + p + 1) * rows] for p in range(5)]
            q = [part[:, :size] for part in own] + [part[:, size:] for part in own]
            r = [target[c] - q[1 + c] for c in range(3)]
            inverse = lax.rsqrt(r[0] * r[0] + r[1] * r[1] + r[2] * r[2] + SOFT2)
            inverse_sq = inverse * inverse
            cube = inverse * inverse_sq
            fifth = cube * inverse_sq
            dot = [
                q[4] * r[0] + q[7] * r[1] + q[8] * r[2],
                q[7] * r[0] + q[5] * r[1] + q[9] * r[2],
                q[8] * r[0] + q[9] * r[1] + q[6] * r[2],
            ]
            form = r[0] * dot[0] + r[1] * dot[1] + r[2] * dot[2]
            scale = q[0] * cube + 2.5 * form * (fifth * inverse_sq)
            for c in range(3):
                total[c] = total[c] + (dot[c] * fifth - scale * r[c])
    return total


class Near:
    def __init__(self, plan, rank_ref, src_ref, lists, face_ref=None):
        self.plan = plan
        self.rank_ref = rank_ref
        self.src_ref = src_ref
        self.lists = lists
        self.face_ref = face_ref

    def one_hot(self, t, first, count):
        slot = lax.broadcasted_iota(jnp.int32, (count, self.plan.size), 0).astype(F32)
        return self.rank_ref[pl.ds(t, 1), :] == slot + first

    def compact(self, t, first, count, values):
        size = self.plan.size
        pick = jnp.where(self.one_hot(t, first, count), 1.0, 0.0).astype(BF16)
        sub = lax.broadcasted_iota(jnp.int32, (8, size), 0)
        own = jnp.broadcast_to(values[-1], (8, size))
        for i in range(len(values) - 2, -1, -1):
            own = jnp.where(sub == i, values[i], own)
        high, middle, low = split3(own)
        return dot_nt(pick, high) + dot_nt(pick, middle) + dot_nt(pick, low)

    def local_rows(self, t):
        found = []
        for s in range(self.plan.kl):
            index = self.lists[0][s, t]
            found.append([self.src_ref[c, pl.ds(index, 1), :] for c in range(4)])
        return found

    def remote_rows(self, t):
        found = []
        for slot in range(3):
            for k in range(self.plan.kn):
                index = self.lists[1][slot, k, t]
                found.append([self.face_ref[slot, c, pl.ds(index, 1), :] for c in range(4)])
        return found

    def pair_sums(self, here, sources, sums=None):
        for source in sources:
            r = [source[c] - here[c] for c in range(3)]
            inverse = lax.rsqrt(r[0] * r[0] + r[1] * r[1] + r[2] * r[2] + SOFT2)
            strength = source[3] * inverse * (inverse * inverse)
            new = [r[c] * strength for c in range(3)]
            sums = new if sums is None else [sums[c] + new[c] for c in range(3)]
        return sums

    def spread(self, packed):
        return [jnp.broadcast_to(packed[:, c : c + 1], (8, self.plan.size)) for c in range(3)]

    def prepare(self, t, comp_ref, wide_ref):
        shape = (FAST_GROUPS * 8, self.plan.size)
        for c in range(3):
            value = jnp.broadcast_to(comp_ref[t, :, pl.ds(c, 1)], shape)
            for g in range(FAST_GROUPS):
                wide_ref[t, g, c] = value[g * 8 : g * 8 + 8]

    def force(self, t, rows, wide_ref, part_ref, init_ref=None):
        for g in range(FAST_GROUPS):
            here = [wide_ref[t, g, c] for c in range(3)]
            sums = None if init_ref is None else [init_ref[t, g, c] for c in range(3)]
            for c, value in enumerate(self.pair_sums(here, rows, sums)):
                part_ref[t, g, c] = value

    def scatter(self, t, part_ref, row_ref):
        out = [None] * 3
        for g in range(FAST_GROUPS):
            mask = self.one_hot(t, g * 8, 8)
            for c in range(3):
                value = jnp.where(mask, lane_sum(part_ref[t, g, c]), 0.0)
                out[c] = value if out[c] is None else out[c] + value
        for c in range(3):
            row_ref[c, pl.ds(t, 1), :] = jnp.sum(out[c], axis=0, keepdims=True)

    def rest(self, row_ref):
        @pl.when(jnp.max(self.rank_ref[...]) >= FAST_GROUPS * 8)
        def _():
            def tile_rest(t, carry):
                def group(g, inner):
                    values = [self.src_ref[c, pl.ds(t, 1), :] for c in range(3)]
                    here = self.spread(self.compact(t, g * 8, 8, values))
                    sums = self.pair_sums(here, self.local_rows(t) + self.remote_rows(t))
                    mask = self.one_hot(t, g * 8, 8)
                    for c in range(3):
                        value = jnp.where(mask, lane_sum(sums[c]), 0.0)
                        old = row_ref[c, pl.ds(t, 1), :]
                        row_ref[c, pl.ds(t, 1), :] = old + jnp.sum(value, axis=0, keepdims=True)
                    return inner

                most = jnp.max(self.rank_ref[pl.ds(t, 1), :]).astype(jnp.int32)
                lax.fori_loop(FAST_GROUPS, (most + 8) // 8, group, 0)
                return carry

            lax.fori_loop(0, self.plan.tiles, tile_rest, 0)


def shift_of(plan, level, bit):
    _, place, _ = plan.place[level]
    span = float(plan.grid * 2**place)
    return jnp.where(bit == 0, span, -span).astype(F32)


def lists_start(ins, outs, sems):
    copies = [pltpu.make_async_copy(ins[i], outs[i], sems.at[i]) for i in range(2)]
    for copy in copies:
        copy.start()

    def arrived():
        for copy in copies:
            copy.wait()
        return outs

    return arrived


def rank_rows(plan, act):
    size = plan.size
    below = lax.broadcasted_iota(jnp.int32, (size, size), 0) < lax.broadcasted_iota(
        jnp.int32, (size, size), 1
    )
    rank = dot_nn(act.astype(BF16), jnp.where(below, 1.0, 0.0).astype(BF16))
    return jnp.where(act > 0, rank, -1.0)


def tile_loop(plan, step):
    def body(i, carry):
        step([jnp.minimum(i * UNROLL + j, plan.tiles - 1) for j in range(UNROLL)])
        return carry

    lax.fori_loop(0, (plan.tiles + UNROLL - 1) // UNROLL, body, 0)


def local_kernel(plan, *refs):
    arrived = lists_start(refs[:2], refs[-3:-1], refs[-1])
    base_ref, far_ref, rank_ref, pick_ref, comp_ref, wide_ref, part_ref = refs[2:9]
    tiles = plan.tiles
    rank_ref[...] = rank_rows(plan, base_ref[7])
    far_picks(plan, far_ref, pick_ref)
    near = Near(plan, rank_ref, base_ref, None)
    for t in range(tiles):
        own = base_ref[7, pl.ds(t, 1), :]
        values = [base_ref[c, pl.ds(t, 1), :] for c in range(3)]
        values += [base_ref[4 + c, pl.ds(t, 1), :] * own for c in range(3)]
        comp_ref[t, :, pl.ds(0, 8)] = near.compact(t, 0, FAST_GROUPS * 8, values)
    for j in range(UNROLL):
        near.prepare(min(j, tiles - 1), comp_ref, wide_ref)
    near.lists = arrived()

    def step(ts):
        for t in ts:
            near.force(t, near.local_rows(t), wide_ref, part_ref)
        for t in ts:
            near.prepare(jnp.minimum(t + UNROLL, tiles - 1), comp_ref, wide_ref)

    tile_loop(plan, step)


def gather_kernel(plan, rank_ref, comp_ref, acc_ref, u_ref, a_ref):
    near = Near(plan, rank_ref, acc_ref, None)
    for t in range(plan.tiles):
        values = [acc_ref[c, pl.ds(t, 1), :] for c in range(3)]
        a_ref[t, :, pl.ds(0, 8)] = near.compact(t, 0, FAST_GROUPS * 8, values)
        u_ref[t] = pltpu.roll(comp_ref[t], plan.size - 3, 1)


def lane_row(plan, level, bit):
    cut, _, _ = plan.place[level]
    lane = lax.broadcasted_iota(jnp.int32, (1, plan.size), 1)
    return jnp.where(lane == 1 + cut, shift_of(plan, level, bit), 0.0)


def square_row(acc):
    square = acc[0] * acc[0] + acc[1] * acc[1] + acc[2] * acc[2]
    return jnp.max(square, axis=0, keepdims=True)


def time_step_of(square):
    return ETA / jnp.sqrt(jnp.sqrt(square) + 1e-06)


def second_kernel(plan, *refs):
    face_ref, part_ref, row_ref, *smem = refs[-6:]
    arrived, refs = lists_start(refs[:2], smem[:2], smem[2]), refs[2:]
    base_ref, pick_ref, rank_ref, wide_ref, init_ref = refs[:5]
    near_refs = refs[5:8]
    extra = plan.levels - 3
    moment_refs = refs[8 : 8 + extra]
    acc_ref, pack_ref = refs[8 + extra : 10 + extra]
    send_refs = refs[10 + extra : 13 + extra]
    rows, tiles = plan.rows, plan.tiles
    bits = device_bits(plan.levels)
    face = plan.face
    for slot in range(3):
        level = plan.near_level[slot]
        cut = plan.place[level][0]
        for c in range(3):
            value = near_refs[slot][pl.ds(c * face, face), :]
            if c == cut:
                value = value + shift_of(plan, level, bits[level])
            face_ref[slot, c, pl.ds(0, face), :] = value
        face_ref[slot, 3, pl.ds(0, face), :] = near_refs[slot][pl.ds(plan.row_m, face), :]
    tables = []
    others = list(moment_refs)
    for level in range(plan.levels):
        slot = plan.place[level][2]
        table = near_refs[slot][pl.ds(plan.row_t, rows), :] if slot >= 0 else others.pop(0)[...]
        tables.append(table + lane_row(plan, level, bits[level]))
    act = base_ref[7]
    position = [base_ref[c] for c in range(3)]
    far = far_field(plan, pick_ref, tables, fold_matrix(plan.size, False), position)
    row_ref[...] = jnp.zeros(row_ref.shape, F32)
    near = Near(plan, rank_ref, base_ref, arrived(), face_ref)

    def step(ts):
        for t in ts:
            near.scatter(jnp.maximum(t - UNROLL, 0), part_ref, row_ref)
        for t in ts:
            near.force(t, near.remote_rows(t), wide_ref, part_ref, init_ref)

    tile_loop(plan, step)
    for j in range(UNROLL):
        near.scatter(max(tiles - 1 - j, 0), part_ref, row_ref)
    near.rest(row_ref)
    acc = [act * (GRAV * (row_ref[c] + far[c])) for c in range(3)]
    for c in range(3):
        acc_ref[c] = acc[c]
    velocity = [base_ref[4 + c] * act for c in range(3)]
    table = moment_table(base_ref[3], [position, velocity, acc], 1)
    pack_ref[...] = pack_table(table, jnp.max(square_row(acc), axis=1, keepdims=True))
    for slot, ref in enumerate(send_refs):
        for s, row in enumerate(face_rows(plan, slot, bits[plan.near_level[slot]])):
            for c in range(3):
                ref[pl.ds(c * face + s, 1), :] = acc_ref[c, pl.ds(row, 1), :]


def third_kernel(plan, *refs):
    face_ref, part_ref, row_ref, src_ref, moved_ref, slot_ref, wide_ref, *smem = refs[-10:]
    arrived, refs = lists_start(refs[:2], smem[:2], smem[2]), refs[2:]
    base_ref, pick_ref, rank_ref, comp_ref, u_ref, a_ref, acc_ref, all_ref = refs[:8]
    near_refs = refs[8:11]
    send_refs = refs[11:14]
    extra = plan.levels - 3
    moment_refs = refs[14 : 14 + extra]
    pos_ref, out_ref, square_ref, step_ref = refs[14 + extra : 18 + extra]
    rows, size, tiles = plan.rows, plan.size, plan.tiles
    bits = device_bits(plan.levels)
    square = jnp.max(all_ref[:, 7, :], axis=0, keepdims=True)
    square = jnp.where(lax.broadcasted_iota(jnp.int32, (1, size), 1) == size - 1, square, 0.0)
    step = time_step_of(jnp.max(square, axis=1, keepdims=True))
    step_ref[...] = jnp.broadcast_to(step, step_ref.shape)
    wide = jnp.broadcast_to(step, (rows, size))
    position = []
    act = base_ref[7]
    for c in range(3):
        moved = base_ref[c] + (base_ref[4 + c] * act + acc_ref[c] * wide) * wide
        pos_ref[c] = moved
        src_ref[c] = moved
        position.append(moved)
    src_ref[3] = base_ref[3]
    slots = jnp.broadcast_to(step, (FAST_GROUPS * 8, size))
    for t in range(tiles):
        slot_ref[t] = comp_ref[t] + (u_ref[t] + a_ref[t] * slots) * slots
    powers = powers_row(step, size)
    device = lax.axis_index(AXES)
    tables = []
    others = list(moment_refs)
    for level in range(plan.levels):
        slot = plan.place[level][2]
        table = near_refs[slot][pl.ds(plan.row_t, rows), :] if slot >= 0 else others.pop(0)[...]
        terms = unpack_table(all_ref[device ^ (1 << level)], rows)
        tables.append(table + lane_row(plan, level, bits[level]) + terms * powers)
    face = plan.face
    frows = plan.frows
    fwide = jnp.broadcast_to(step, (frows, size))
    for slot in range(3):
        level = plan.near_level[slot]
        cut = plan.place[level][0]
        got = near_refs[slot]
        moved_ref[slot] = (
            got[pl.ds(0, frows), :]
            + (got[pl.ds(plan.row_u, frows), :] + send_refs[slot][pl.ds(0, frows), :] * fwide)
            * fwide
        )
        for c in range(3):
            value = moved_ref[slot, pl.ds(c * face, face), :]
            if c == cut:
                value = value + shift_of(plan, level, bits[level])
            face_ref[slot, c, pl.ds(0, face), :] = value
        face_ref[slot, 3, pl.ds(0, face), :] = got[pl.ds(plan.row_m, face), :]
    far = far_field(plan, pick_ref, tables, fold_matrix(size, True), position)
    row_ref[...] = jnp.zeros(row_ref.shape, F32)
    near = Near(plan, rank_ref, src_ref, arrived(), face_ref)
    for j in range(UNROLL):
        near.prepare(min(j, tiles - 1), slot_ref, wide_ref)

    def work(ts):
        for t in ts:
            near.scatter(jnp.maximum(t - UNROLL, 0), part_ref, row_ref)
        for t in ts:
            near.force(t, near.local_rows(t) + near.remote_rows(t), wide_ref, part_ref)
        for t in ts:
            near.prepare(jnp.minimum(t + UNROLL, tiles - 1), slot_ref, wide_ref)

    tile_loop(plan, work)
    for j in range(UNROLL):
        near.scatter(max(tiles - 1 - j, 0), part_ref, row_ref)
    near.rest(row_ref)
    acc = [act * (GRAV * (row_ref[c] + far[c])) for c in range(3)]
    for c in range(3):
        out_ref[c] = acc[c]
    square_ref[...] = square_row(acc)


def last_kernel(plan, max_ref, base_ref, pos_ref, first_ref, acc_ref, step_ref,
                pos_out, vel_out, acc_out, steps_out, work_ref):
    rows, size = plan.rows, plan.size
    second = time_step_of(jnp.max(max_ref[...], axis=(0, 1), keepdims=True))
    one = step_ref[...]
    steps_out[0] = one[0, 0]
    steps_out[1] = second[0, 0]
    first = jnp.broadcast_to(one[:, :1], (rows, size))
    wide = jnp.broadcast_to(second, (rows, size))
    act = base_ref[7]
    for c in range(3):
        velocity = base_ref[4 + c] + first_ref[c] * first + acc_ref[c] * wide
        work_ref[0, c] = pos_ref[c] + velocity * act * wide
        work_ref[1, c] = velocity
    for t in range(plan.tiles):
        lanes = pl.ds(t * size, size)
        for c in range(3):
            pos_out[pl.ds(c, 1), lanes] = work_ref[0, c, pl.ds(t, 1), :]
            vel_out[pl.ds(c, 1), lanes] = work_ref[1, c, pl.ds(t, 1), :]
            acc_out[pl.ds(c, 1), lanes] = acc_ref[c, pl.ds(t, 1), :]


def vmem():
    return pl.BlockSpec(memory_space=pltpu.VMEM)


def hbm():
    return pl.BlockSpec(memory_space=pltpu.HBM)


def in_hbm(values):
    return pltpu.with_memory_space_constraint(values, pltpu.HBM)


def smem():
    return pl.BlockSpec(memory_space=pltpu.SMEM)


def call(kernel, outs, scratch, specs, name, out_specs=None):
    return pl.pallas_call(
        kernel,
        out_shape=outs,
        in_specs=specs,
        out_specs=out_specs or [vmem() for _ in outs],
        scratch_shapes=scratch,
        compiler_params=pltpu.CompilerParams(vmem_limit_bytes=VMEM_BYTES),
        name=name,
    )


def buffers(*shapes):
    return [pltpu.VMEM(shape, F32) for shape in shapes]


def floats(*shapes):
    return [jax.ShapeDtypeStruct(shape, F32) for shape in shapes]


def exchange(plan, block, bits):
    flip = sum(1 << bit for bit in bits)
    return lax.ppermute(block, AXES, [(i, i ^ flip) for i in range(plan.devices)])


def body(mesh, offsets, velocities, masses, active, near_local, near_remote, far_list):
    tiles, kl = near_local.shape
    kn = near_remote.shape[2]
    levels, km = far_list.shape[1:]
    size = masses.shape[0] // tiles
    plan = Plan(mesh, tiles, size, levels, km, kl, kn)
    rows, near_rows = plan.rows, plan.near_rows
    whole = (3, rows, size)
    extra = levels - 3
    base, moments, far_ids, *near = call(
        functools.partial(first_kernel, plan),
        floats((8, rows, size), (rows, size))
        + [jax.ShapeDtypeStruct((rows, size), jnp.int32)]
        + floats(*[(near_rows, size)] * 3),
        buffers(offsets.shape, velocities.shape, (tiles, size))
        + [
            pltpu.VMEM((tiles, size), jnp.int32),
            pltpu.VMEM((levels, km, tiles), jnp.int32),
            pltpu.SemaphoreType.DMA((5,)),
        ],
        [hbm()] * 5,
        "first",
    )(
        in_hbm(offsets),
        in_hbm(velocities),
        in_hbm(masses.reshape(tiles, size)),
        in_hbm(active.reshape(tiles, size)),
        in_hbm(jnp.transpose(far_list, (1, 2, 0))),
    )

    got_near = [None] * 3
    got_far = []
    for slot in range(3):
        got_near[slot] = exchange(plan, near[slot], [plan.near_level[slot]])
    for level in range(levels):
        if plan.place[level][2] < 0:
            got_far.append(exchange(plan, moments, [level]))

    lists = (
        in_hbm(jnp.transpose(near_local)),
        in_hbm(jnp.transpose(near_remote, (1, 2, 0))),
    )
    slots = (tiles, FAST_GROUPS * 8, size)
    broad = (tiles, FAST_GROUPS, 3, 8, size)
    list_scratch = [
        pltpu.SMEM((kl, tiles), jnp.int32),
        pltpu.SMEM((3, kn, tiles), jnp.int32),
        pltpu.SemaphoreType.DMA((2,)),
    ]
    force_scratch = buffers((3, 4, up8(plan.face), size), broad, whole)
    rank, picks, comp, spread, local = call(
        functools.partial(local_kernel, plan),
        floats((rows, size))
        + [jax.ShapeDtypeStruct((levels * km, rows, size), BF16)]
        + floats(slots, broad, broad),
        list_scratch,
        [hbm(), hbm(), vmem(), vmem()],
        "local",
    )(*lists, base, far_ids)
    acc, packed, *send = call(
        functools.partial(second_kernel, plan),
        floats(whole, (8, size), *[(plan.frows, size)] * 3),
        force_scratch + list_scratch,
        [hbm(), hbm()] + [vmem()] * (5 + levels),
        "second",
    )(*lists, base, picks, rank, spread, local, *got_near, *got_far)
    slot_u, slot_a = call(
        functools.partial(gather_kernel, plan),
        floats(slots, slots),
        [],
        [vmem()] * 3,
        "gather",
    )(rank, comp, acc)

    got_send = [exchange(plan, send[slot], [plan.near_level[slot]]) for slot in range(3)]
    everyone = lax.all_to_all(
        jnp.broadcast_to(packed[None], (plan.devices, 8, size)), AXES, 0, 0
    )
    moved, acc2, square2, step = call(
        functools.partial(third_kernel, plan),
        floats(whole, whole, (1, size), (1, size)),
        force_scratch
        + buffers((4, rows, size), (3, plan.frows, size), slots, broad)
        + list_scratch,
        [hbm(), hbm()] + [vmem()] * (8 + 3 + 3 + extra),
        "third",
    )(
        *lists, base, picks, rank, comp, slot_u, slot_a, acc, everyone, *got_near, *got_send, *got_far,
    )
    copies = jnp.broadcast_to(square2[None], (plan.devices, 1, size))
    largest = lax.all_to_all(copies, AXES, 0, 0).reshape(plan.devices, size)
    pos, vel, out, steps = call(
        functools.partial(last_kernel, plan),
        floats(offsets.shape, offsets.shape, offsets.shape, (SUBSTEPS,)),
        buffers((2, 3, rows, size)),
        [vmem()] * 6,
        "last",
        [vmem(), vmem(), vmem(), smem()],
    )(largest, base, moved, acc, acc2, step)
    return pos, vel, out, steps


def solution(mesh):
    parts = P(None, AXES)
    return jax.shard_map(
        functools.partial(body, mesh),
        mesh=mesh,
        in_specs=(parts, parts, P(AXES), P(AXES), P(AXES, None), P(AXES, None, None), P(AXES, None, None)),
        out_specs=(parts, parts, parts, P()),
        check_vma=False,
    )
```

```python
import functools

import jax
import jax.numpy as jnp
from jax import lax
from jax.experimental import pallas as pl
from jax.experimental.pallas import tpu as pltpu
from jax.sharding import PartitionSpec as P

SUBSTEPS = 2
GRAV = 0.02
SOFT2 = 0.0025
ETA = 0.15
AXES = ("gx", "gy", "gz")
F32 = jnp.float32
BF16 = jnp.bfloat16
FAST_GROUPS = 6
VMEM_BYTES = 16 * 2**20


def up8(count):
    return (count + 7) // 8 * 8


def level_place(level, z_bits, y_bits):
    if level < z_bits:
        return (2, level, 0 if level == 0 else -1)
    if level < z_bits + y_bits:
        return (1, level - z_bits, 1 if level == z_bits else -1)
    return (0, level - z_bits - y_bits, 2 if level == z_bits + y_bits else -1)


class Plan:
    def __init__(self, mesh, count_tiles, tile_size, levels, km, kl, kn):
        self.tiles = count_tiles
        self.size = tile_size
        self.rows = up8(count_tiles)
        self.unroll = 3 if count_tiles % 3 == 0 else 1
        self.grid = round(count_tiles ** (1 / 3))
        self.face = self.grid * self.grid
        self.levels = levels
        self.km = km
        self.kl = kl
        self.kn = kn
        self.devices = mesh.size
        z_bits = mesh.shape["gz"].bit_length() - 1
        y_bits = mesh.shape["gy"].bit_length() - 1
        self.place = [level_place(level, z_bits, y_bits) for level in range(levels)]
        self.near_level = [None] * 3
        for level, (_, _, slot) in enumerate(self.place):
            if slot >= 0:
                self.near_level[slot] = level
        self.frows = up8(3 * self.face)
        self.row_u = self.frows
        self.row_m = 2 * self.frows
        self.row_t = self.row_m + up8(self.face)
        self.near_rows = self.row_t + self.rows


def lane_sum(values):
    return jnp.sum(values, axis=1, keepdims=True)


def split3(values):
    high = values.astype(BF16)
    rest = values - high.astype(F32)
    middle = rest.astype(BF16)
    low = (rest - middle.astype(F32)).astype(BF16)
    return high, middle, low


def dot_nt(left, right):
    return lax.dot_general(left, right, (((1,), (1,)), ((), ())), preferred_element_type=F32)


def dot_nn(left, right):
    return lax.dot_general(left, right, (((1,), (0,)), ((), ())), preferred_element_type=F32)


PAIRS = ((0, 0), (1, 1), (2, 2), (0, 1), (0, 2), (1, 2))


def spread_sums(blocks):
    rows, size = blocks[0].shape
    tall = blocks[0] if len(blocks) == 1 else jnp.concatenate(blocks, axis=0)
    high = tall.astype(BF16)
    rest = (tall - high.astype(F32)).astype(BF16)
    sums = dot_nn(jnp.concatenate([high, rest], axis=1), jnp.ones((2 * size, size), BF16))
    return [sums[i * rows : (i + 1) * rows] for i in range(len(blocks))]


def lane_of(k, p):
    if k == 0:
        return (8, 6, 7, 22, 0, 1, 2, 3, 4, 5)[p]
    return 8 * (k - 1) + p - 4 if p > 3 else (6, 7, 22)[p - 1] + 8 * (k - 1)


def moment_table(mass, parts, low):
    shape = mass.shape
    lane = lax.broadcasted_iota(jnp.int32, shape, 1)
    count = len(parts)
    total, *firsts = spread_sums([mass] + [mass * part[c] for part in parts for c in range(3)])
    columns = [(0, 0, total)]
    rel = []
    for k, part in enumerate(parts):
        line = []
        for c in range(3):
            center = firsts[3 * k + c] / total
            columns.append((k, 1 + c, center))
            line.append(part[c] - center)
        rel.append(line)
    weighted = [[mass * line[c] for c in range(3)] for line in rel]
    terms = []
    for k in range(low, 2 * count - 1):
        for a, b in PAIRS:
            term = None
            for i in range(count):
                j = k - i
                if 0 <= j < count:
                    item = weighted[i][a] * rel[j][b]
                    term = item if term is None else term + item
            terms.append(term)
    seconds = spread_sums(terms)
    for k in range(low, 2 * count - 1):
        second = seconds[6 * (k - low) : 6 * (k - low) + 6]
        trace = second[0] + second[1] + second[2]
        for q in range(6):
            value = 3.0 * second[q] - trace if q < 3 else 3.0 * second[q]
            columns.append((k, 4 + q, value))
    table = jnp.zeros(shape, F32)
    for k, p, value in columns:
        if low <= k and (k > 0 or low == 0):
            table = jnp.where(lane == lane_of(k, p), value, table)
    return table


def moment_rows(size):
    row = lax.broadcasted_iota(jnp.int32, (16, size), 0)
    lane = lax.broadcasted_iota(jnp.int32, (16, size), 1)
    hit = None
    for p in range(10):
        one = (row == p) & (lane == lane_of(0, p))
        hit = one if hit is None else hit | one
    return jnp.where(hit, 1.0, 0.0).astype(BF16)


def powers_row(step, size, width):
    lane = lax.broadcasted_iota(jnp.int32, (1, size), 1) % width
    out = jnp.zeros((1, size), F32)
    power = step
    for k in range(1, 5):
        hit = None
        for p in range(1, 10):
            if p > 3 or k < 3:
                one = lane == lane_of(k, p)
                hit = one if hit is None else hit | one
        out = jnp.where(hit, power, out)
        power = power * step
    return out


def pack_table(table, square):
    rows, size = table.shape
    blocks = rows // 8
    width = size // blocks
    row = lax.broadcasted_iota(jnp.int32, (8, size), 0)
    lane = lax.broadcasted_iota(jnp.int32, (8, size), 1)
    out = table[:8]
    for j in range(1, blocks):
        out = jnp.where(lane < j * width, out, pltpu.roll(table[8 * j : 8 * j + 8], j * width, 1))
    return jnp.where((row == 7) & (lane >= size - width), square, out)


def unpack_table(packed, powers, rows):
    size = packed.shape[1]
    blocks = rows // 8
    width = size // blocks
    lane = lax.broadcasted_iota(jnp.int32, (8, size), 1)
    terms = packed * powers
    twice = terms + pltpu.roll(terms, size - 8, 1)
    four = twice + pltpu.roll(twice, size - 16, 1)
    folded = jnp.where(lane % width < 6, four, twice)
    keep = (lane < 8) | (lane == lane_of(0, 3))
    parts = [pltpu.roll(folded, size - j * width, 1) if j else folded for j in range(blocks)]
    return jnp.concatenate([jnp.where(keep, part, 0.0) for part in parts], axis=0)


def device_bits(levels):
    device = lax.axis_index(AXES)
    return [jnp.right_shift(device, level) & 1 for level in range(levels)]


def face_rows(plan, slot, bit):
    cut = 2 - slot
    grid = plan.grid
    strides = (grid * grid, grid, 1)
    others = [axis for axis in range(3) if axis != cut]
    coord = jnp.where(bit == 1, 0, grid - 1)
    base = coord * strides[cut]
    return [
        base + s // grid * strides[others[0]] + s % grid * strides[others[1]]
        for s in range(plan.face)
    ]


def first_kernel(plan, *refs):
    ins, (base_ref, mom_ref, id_ref), near_refs = refs[:5], refs[5:8], refs[8:11]
    buffers, sems = refs[11:16], refs[16]
    copies = [pltpu.make_async_copy(ins[i], buffers[i], sems.at[i]) for i in range(5)]
    for copy in copies:
        copy.start()
    for copy in copies:
        copy.wait()
    off_ref, vel_ref, mass_ref, act_ref, far_ref = buffers
    tiles, rows, size, grid = plan.tiles, plan.rows, plan.size, plan.grid
    tile = lax.broadcasted_iota(jnp.int32, (rows, size), 0)
    base_ref[...] = jnp.zeros(base_ref.shape, F32)
    for t in range(tiles):
        lanes = pl.ds(t * size, size)
        for c in range(3):
            base_ref[c, pl.ds(t, 1), :] = off_ref[pl.ds(c, 1), lanes]
            base_ref[4 + c, pl.ds(t, 1), :] = vel_ref[pl.ds(c, 1), lanes]
    base_ref[3, pl.ds(0, tiles), :] = mass_ref[...]
    base_ref[7, pl.ds(0, tiles), :] = act_ref[...].astype(F32)
    corners = (tile // (grid * grid), tile // grid % grid, tile % grid)
    inside = tile < tiles
    act = base_ref[7]
    position = []
    for c in range(3):
        value = jnp.where(inside, base_ref[c] + corners[c].astype(F32), 0.0)
        base_ref[c] = value
        position.append(value)
    mass = jnp.where(inside, base_ref[3], 1.0)
    base_ref[3] = mass
    table = moment_table(mass, [position], 0)
    mom_ref[...] = table
    lists = plan.levels * plan.km
    flat = jnp.concatenate(
        [far_ref[level].astype(F32) for level in range(plan.levels)]
        + [jnp.zeros((up8(lists) - lists, tiles), F32)] * (lists % 8 > 0),
        axis=0,
    )
    id_ref[pl.ds(0, tiles), pl.ds(0, up8(lists))] = jnp.transpose(flat).astype(jnp.int32)
    bits = device_bits(plan.levels)
    for slot, ref in enumerate(near_refs):
        ref[pl.ds(plan.row_t, rows), :] = table
        for s, row in enumerate(face_rows(plan, slot, bits[plan.near_level[slot]])):
            for c in range(3):
                ref[pl.ds(c * plan.face + s, 1), :] = base_ref[c, pl.ds(row, 1), :]
                ref[pl.ds(plan.row_u + c * plan.face + s, 1), :] = (
                    base_ref[4 + c, pl.ds(row, 1), :] * base_ref[7, pl.ds(row, 1), :]
                )
            ref[pl.ds(plan.row_m + s, 1), :] = base_ref[3, pl.ds(row, 1), :]


def far_picks(plan, far_ref, pick_ref):
    rows, size = plan.rows, plan.size
    lane = lax.broadcasted_iota(jnp.int32, (rows, size), 1)
    ids = far_ref[...].astype(F32)
    items = plan.levels * plan.km
    tall = jnp.concatenate([jnp.where(lane == i, ids, 0.0) for i in range(items)], axis=0)
    spread = dot_nn(tall.astype(BF16), jnp.ones((size, size), BF16))
    cell = jnp.where(lane < 3 * rows, lane % rows, -1).astype(F32)
    for i in range(items):
        hit = spread[i * rows : (i + 1) * rows] == cell
        pick_ref[i] = jnp.where(hit, 1.0, 0.0).astype(BF16)


def far_field(plan, pick_ref, tables, target):
    rows, size, km = plan.rows, plan.size, plan.km
    total = [jnp.zeros((rows, size), F32) for _ in range(3)]
    one = moment_rows(size)
    blank = jnp.zeros((size - 3 * rows, size), BF16)
    half = lax.broadcasted_iota(jnp.int32, (2 * size, 2 * size), 0) < size
    left = lax.broadcasted_iota(jnp.int32, (2 * size, 2 * size), 1) < size
    ones = jnp.where(half == left, 1.0, 0.0).astype(BF16)
    tall = []
    for level in range(plan.levels):
        flat = dot_nt(one, jnp.concatenate([*split3(tables[level]), blank], axis=0)).astype(BF16)
        wide = [jnp.broadcast_to(flat[p : p + 1], (rows, size)) for p in range(10)]
        for k in range(km):
            pick = pick_ref[level * km + k]
            tall += [
                jnp.concatenate([pick * wide[p], pick * wide[p + 5]], axis=1) for p in range(5)
            ]
    got = dot_nn(jnp.concatenate(tall, axis=0), ones)
    for item in range(plan.levels * km):
        own = [got[(5 * item + p) * rows : (5 * item + p + 1) * rows] for p in range(5)]
        q = [part[:, :size] for part in own] + [part[:, size:] for part in own]
        r = [target[c] - q[1 + c] for c in range(3)]
        inverse = lax.rsqrt(r[0] * r[0] + r[1] * r[1] + r[2] * r[2] + SOFT2)
        inverse_sq = inverse * inverse
        cube = inverse * inverse_sq
        fifth = cube * inverse_sq
        dot = [
            q[4] * r[0] + q[7] * r[1] + q[8] * r[2],
            q[7] * r[0] + q[5] * r[1] + q[9] * r[2],
            q[8] * r[0] + q[9] * r[1] + q[6] * r[2],
        ]
        form = r[0] * dot[0] + r[1] * dot[1] + r[2] * dot[2]
        scale = q[0] * cube + 2.5 * form * (fifth * inverse_sq)
        for c in range(3):
            total[c] = total[c] + (dot[c] * fifth - scale * r[c])
    return total


class Near:
    def __init__(self, plan, rank_ref, src_ref, lists, face_ref=None):
        self.plan = plan
        self.rank_ref = rank_ref
        self.src_ref = src_ref
        self.lists = lists
        self.face_ref = face_ref

    def tile(self, p):
        return self.lists[2][0, p] if len(self.lists) > 2 else p

    def one_hot(self, t, first, count):
        slot = lax.broadcasted_iota(jnp.int32, (count, self.plan.size), 0).astype(F32)
        return self.rank_ref[pl.ds(t, 1), :] == slot + first

    def compact(self, t, first, count, values):
        size = self.plan.size
        pick = jnp.where(self.one_hot(t, first, count), 1.0, 0.0).astype(BF16)
        sub = lax.broadcasted_iota(jnp.int32, (8, size), 0)
        own = jnp.broadcast_to(values[-1], (8, size))
        for i in range(len(values) - 2, -1, -1):
            own = jnp.where(sub == i, values[i], own)
        high, middle, low = split3(own)
        return dot_nt(pick, high) + dot_nt(pick, middle) + dot_nt(pick, low)

    def local_rows(self, t):
        found = []
        for s in range(self.plan.kl):
            index = self.lists[0][s, t]
            found.append([self.src_ref[c, pl.ds(index, 1), :] for c in range(4)])
        return found

    def remote_rows(self, t):
        found = []
        for slot in range(3):
            for k in range(self.plan.kn):
                index = self.lists[1][slot, k, t]
                found.append([self.face_ref[slot, c, pl.ds(index, 1), :] for c in range(4)])
        return found

    def pair_sums(self, here, sources, sums=None):
        for source in sources:
            r = [source[c] - here[c] for c in range(3)]
            inverse = lax.rsqrt(r[0] * r[0] + r[1] * r[1] + r[2] * r[2] + SOFT2)
            strength = source[3] * inverse * (inverse * inverse)
            new = [r[c] * strength for c in range(3)]
            sums = new if sums is None else [sums[c] + new[c] for c in range(3)]
        return sums

    def spread(self, packed):
        return [jnp.broadcast_to(packed[:, c : c + 1], (8, self.plan.size)) for c in range(3)]

    def prepare(self, p, groups, comp_ref, wide_ref):
        t = self.tile(p)
        count = groups * 8
        for c in range(3):
            column = comp_ref[t, pl.ds(0, count), pl.ds(c, 1)]
            wide_ref[t, c, pl.ds(0, count), :] = jnp.broadcast_to(column, (count, self.plan.size))

    def force(self, p, groups, find, wide_ref, part_ref, init_ref=None):
        t = self.tile(p)
        rows = find(t)
        for g in range(groups):
            block = pl.ds(g * 8, 8)
            here = [wide_ref[t, c, block, :] for c in range(3)]
            sums = None if init_ref is None else [init_ref[t, c, block, :] for c in range(3)]
            for c, value in enumerate(self.pair_sums(here, rows, sums)):
                part_ref[t, c, block, :] = value

    def scatter(self, p, groups, part_ref, row_ref):
        t = self.tile(p)
        mask = self.one_hot(t, 0, groups * 8)
        for c in range(3):
            value = jnp.where(mask, lane_sum(part_ref[t, c, pl.ds(0, groups * 8), :]), 0.0)
            out = value[:8]
            for g in range(1, groups):
                out = out + value[g * 8 : g * 8 + 8]
            row_ref[c, pl.ds(t, 1), :] = jnp.sum(out, axis=0, keepdims=True)

    def rest(self, row_ref):
        @pl.when(jnp.max(self.rank_ref[...]) >= FAST_GROUPS * 8)
        def _():
            def tile_rest(t, carry):
                def group(g, inner):
                    values = [self.src_ref[c, pl.ds(t, 1), :] for c in range(3)]
                    here = self.spread(self.compact(t, g * 8, 8, values))
                    sums = self.pair_sums(here, self.local_rows(t) + self.remote_rows(t))
                    mask = self.one_hot(t, g * 8, 8)
                    for c in range(3):
                        value = jnp.where(mask, lane_sum(sums[c]), 0.0)
                        old = row_ref[c, pl.ds(t, 1), :]
                        row_ref[c, pl.ds(t, 1), :] = old + jnp.sum(value, axis=0, keepdims=True)
                    return inner

                most = jnp.max(self.rank_ref[pl.ds(t, 1), :]).astype(jnp.int32)
                lax.fori_loop(FAST_GROUPS, (most + 8) // 8, group, 0)
                return carry

            lax.fori_loop(0, self.plan.tiles, tile_rest, 0)


def shift_of(plan, level, bit):
    _, place, _ = plan.place[level]
    span = float(plan.grid * 2**place)
    return jnp.where(bit == 0, span, -span).astype(F32)


def lists_start(ins, outs, sems):
    copies = [pltpu.make_async_copy(a, b, sems.at[i]) for i, (a, b) in enumerate(zip(ins, outs))]
    for copy in copies:
        copy.start()

    def arrived():
        for copy in copies:
            copy.wait()
        return outs

    return arrived


def rank_rows(plan, act):
    size = plan.size
    below = lax.broadcasted_iota(jnp.int32, (size, size), 0) < lax.broadcasted_iota(
        jnp.int32, (size, size), 1
    )
    rank = dot_nn(act.astype(BF16), jnp.where(below, 1.0, 0.0).astype(BF16))
    return jnp.where(act > 0, rank, -1.0)


def tile_order(act, tiles):
    rows, size = act.shape
    act = act.astype(BF16)
    column = dot_nn(act, jnp.ones((size, size), BF16))
    row = dot_nt(jnp.ones((rows, size), BF16), jnp.concatenate([act] * (size // rows), axis=0))
    sub = lax.broadcasted_iota(jnp.int32, (rows, size), 0)
    lane = lax.broadcasted_iota(jnp.int32, (rows, size), 1)
    ahead = (row > column) | ((row == column) & (lane < sub))
    place = lane_sum(jnp.where(ahead & (lane < tiles), 1.0, 0.0))
    here = (place == lane.astype(F32)) & (sub < tiles)
    order = jnp.sum(jnp.where(here, sub.astype(F32), 0.0), axis=0, keepdims=True)
    count = jnp.sum(jnp.where(here, column, 0.0), axis=0, keepdims=True)
    out = lax.broadcasted_iota(jnp.int32, (8, size), 0)
    return jnp.where(out == 0, order, count).astype(jnp.int32)


def tile_loop(plan, order_ref, step):
    few = FAST_GROUPS - 2

    def body(i, carry):
        ps = [i * plan.unroll + j for j in range(plan.unroll)]
        need = (order_ref[1, jnp.maximum(ps[0] - plan.unroll, 0)] + 7) // 8
        for groups in range(few, FAST_GROUPS + 1):
            if groups == few:
                fits = need <= few
            elif groups == FAST_GROUPS:
                fits = need >= groups
            else:
                fits = need == groups

            @pl.when(fits)
            def _(groups=groups):
                step(i, ps, groups)

        return carry

    lax.fori_loop(0, plan.tiles // plan.unroll, body, 0)


def local_kernel(plan, *refs):
    arrived = lists_start(refs[:2], refs[-3:-1], refs[-1])
    base_ref, far_ref, rank_ref, pick_ref, order_ref, comp_ref, wide_ref, part_ref = refs[2:10]
    tiles, groups = plan.tiles, FAST_GROUPS
    rank_ref[...] = rank_rows(plan, base_ref[7])
    far_picks(plan, far_ref, pick_ref)
    order_ref[...] = tile_order(base_ref[7], tiles)
    near = Near(plan, rank_ref, base_ref, refs[-3:-1])
    for t in range(tiles):
        own = base_ref[7, pl.ds(t, 1), :]
        values = [base_ref[c, pl.ds(t, 1), :] for c in range(3)]
        values += [base_ref[4 + c, pl.ds(t, 1), :] * own for c in range(3)]
        comp_ref[t, :, pl.ds(0, 8)] = near.compact(t, 0, groups * 8, values)
    for j in range(plan.unroll):
        near.prepare(j, groups, comp_ref, wide_ref)
    arrived()

    def body(i, carry):
        ps = [i * plan.unroll + j for j in range(plan.unroll)]
        for p in ps:
            near.force(p, groups, near.local_rows, wide_ref, part_ref)
        for p in ps:
            near.prepare(jnp.minimum(p + plan.unroll, tiles - 1), groups, comp_ref, wide_ref)
        return carry

    lax.fori_loop(0, tiles // plan.unroll, body, 0)


def gather_kernel(plan, rank_ref, comp_ref, acc_ref, u_ref, a_ref):
    near = Near(plan, rank_ref, acc_ref, None)
    for t in range(plan.tiles):
        values = [acc_ref[c, pl.ds(t, 1), :] for c in range(3)]
        a_ref[t, :, pl.ds(0, 8)] = near.compact(t, 0, FAST_GROUPS * 8, values)
        u_ref[t] = pltpu.roll(comp_ref[t], plan.size - 3, 1)


def lane_row(plan, level, bit):
    cut, _, _ = plan.place[level]
    lane = lax.broadcasted_iota(jnp.int32, (1, plan.size), 1)
    return jnp.where(lane == lane_of(0, 1 + cut), shift_of(plan, level, bit), 0.0)


def square_row(acc):
    square = acc[0] * acc[0] + acc[1] * acc[1] + acc[2] * acc[2]
    return jnp.max(square, axis=0, keepdims=True)


def time_step_of(square):
    return ETA / jnp.sqrt(jnp.sqrt(square) + 1e-06)


def second_kernel(plan, *refs):
    face_ref, part_ref, row_ref, *smem = refs[-7:]
    arrived, refs = lists_start(refs[:3], smem[:3], smem[3]), refs[3:]
    base_ref, pick_ref, rank_ref, wide_ref, init_ref = refs[:5]
    near_refs = refs[5:8]
    extra = plan.levels - 3
    moment_refs = refs[8 : 8 + extra]
    acc_ref, pack_ref = refs[8 + extra : 10 + extra]
    send_refs = refs[10 + extra : 13 + extra]
    rows, tiles = plan.rows, plan.tiles
    bits = device_bits(plan.levels)
    face = plan.face
    for slot in range(3):
        level = plan.near_level[slot]
        cut = plan.place[level][0]
        for c in range(3):
            value = near_refs[slot][pl.ds(c * face, face), :]
            if c == cut:
                value = value + shift_of(plan, level, bits[level])
            face_ref[slot, c, pl.ds(0, face), :] = value
        face_ref[slot, 3, pl.ds(0, face), :] = near_refs[slot][pl.ds(plan.row_m, face), :]
    tables = []
    others = list(moment_refs)
    for level in range(plan.levels):
        slot = plan.place[level][2]
        table = near_refs[slot][pl.ds(plan.row_t, rows), :] if slot >= 0 else others.pop(0)[...]
        tables.append(table + lane_row(plan, level, bits[level]))
    act = base_ref[7]
    position = [base_ref[c] for c in range(3)]
    far = far_field(plan, pick_ref, tables, position)
    row_ref[...] = jnp.zeros(row_ref.shape, F32)
    near = Near(plan, rank_ref, base_ref, arrived(), face_ref)

    def step(i, ps, groups):
        for p in ps:
            near.scatter(jnp.maximum(p - plan.unroll, 0), groups, part_ref, row_ref)
        for p in ps:
            near.force(p, groups, near.remote_rows, wide_ref, part_ref, init_ref)

    tile_loop(plan, smem[2], step)
    for j in range(plan.unroll):
        near.scatter(tiles - 1 - j, FAST_GROUPS, part_ref, row_ref)
    near.rest(row_ref)
    acc = [act * (GRAV * (row_ref[c] + far[c])) for c in range(3)]
    for c in range(3):
        acc_ref[c] = acc[c]
    velocity = [base_ref[4 + c] * act for c in range(3)]
    table = moment_table(base_ref[3], [position, velocity, acc], 1)
    pack_ref[...] = pack_table(table, jnp.max(square_row(acc), axis=1, keepdims=True))
    for slot, ref in enumerate(send_refs):
        for s, row in enumerate(face_rows(plan, slot, bits[plan.near_level[slot]])):
            for c in range(3):
                ref[pl.ds(c * face + s, 1), :] = acc_ref[c, pl.ds(row, 1), :]


def third_kernel(plan, *refs):
    face_ref, part_ref, row_ref, src_ref, moved_ref, slot_ref, wide_ref, *smem = refs[-11:]
    arrived, refs = lists_start(refs[:3], smem[:3], smem[3]), refs[3:]
    base_ref, pick_ref, rank_ref, comp_ref, u_ref, a_ref, acc_ref, all_ref = refs[:8]
    near_refs = refs[8:11]
    send_refs = refs[11:14]
    extra = plan.levels - 3
    moment_refs = refs[14 : 14 + extra]
    pos_ref, out_ref, square_ref, step_ref = refs[14 + extra : 18 + extra]
    rows, size, tiles = plan.rows, plan.size, plan.tiles
    bits = device_bits(plan.levels)
    square = jnp.max(all_ref[:, 7, :], axis=0, keepdims=True)
    square = jnp.where(lax.broadcasted_iota(jnp.int32, (1, size), 1) == size - 1, square, 0.0)
    step = time_step_of(jnp.max(square, axis=1, keepdims=True))
    step_ref[...] = jnp.broadcast_to(step, step_ref.shape)
    wide = jnp.broadcast_to(step, (rows, size))
    position = []
    act = base_ref[7]
    for c in range(3):
        moved = base_ref[c] + (base_ref[4 + c] * act + acc_ref[c] * wide) * wide
        pos_ref[c] = moved
        src_ref[c] = moved
        position.append(moved)
    src_ref[3] = base_ref[3]
    slots = jnp.broadcast_to(step, (FAST_GROUPS * 8, size))
    for t in range(tiles):
        slot_ref[t] = comp_ref[t] + (u_ref[t] + a_ref[t] * slots) * slots
    powers = powers_row(step, size, 8 * size // rows)
    device = lax.axis_index(AXES)
    tables = []
    others = list(moment_refs)
    for level in range(plan.levels):
        slot = plan.place[level][2]
        table = near_refs[slot][pl.ds(plan.row_t, rows), :] if slot >= 0 else others.pop(0)[...]
        added = unpack_table(all_ref[device ^ (1 << level)], powers, rows)
        tables.append(table + lane_row(plan, level, bits[level]) + added)
    face = plan.face
    frows = plan.frows
    fwide = jnp.broadcast_to(step, (frows, size))
    for slot in range(3):
        level = plan.near_level[slot]
        cut = plan.place[level][0]
        got = near_refs[slot]
        moved_ref[slot] = (
            got[pl.ds(0, frows), :]
            + (got[pl.ds(plan.row_u, frows), :] + send_refs[slot][pl.ds(0, frows), :] * fwide)
            * fwide
        )
        for c in range(3):
            value = moved_ref[slot, pl.ds(c * face, face), :]
            if c == cut:
                value = value + shift_of(plan, level, bits[level])
            face_ref[slot, c, pl.ds(0, face), :] = value
        face_ref[slot, 3, pl.ds(0, face), :] = got[pl.ds(plan.row_m, face), :]
    far = far_field(plan, pick_ref, tables, position)
    row_ref[...] = jnp.zeros(row_ref.shape, F32)
    near = Near(plan, rank_ref, src_ref, arrived(), face_ref)
    for j in range(plan.unroll):
        near.prepare(j, FAST_GROUPS, slot_ref, wide_ref)

    def every_row(t):
        return near.local_rows(t) + near.remote_rows(t)

    def work(i, ps, groups):
        for p in ps:
            near.scatter(jnp.maximum(p - plan.unroll, 0), groups, part_ref, row_ref)
        for p in ps:
            near.force(p, groups, every_row, wide_ref, part_ref)
        for p in ps:
            near.prepare(jnp.minimum(p + plan.unroll, tiles - 1), groups, slot_ref, wide_ref)

    tile_loop(plan, smem[2], work)
    for j in range(plan.unroll):
        near.scatter(tiles - 1 - j, FAST_GROUPS, part_ref, row_ref)
    near.rest(row_ref)
    acc = [act * (GRAV * (row_ref[c] + far[c])) for c in range(3)]
    for c in range(3):
        out_ref[c] = acc[c]
    square_ref[...] = square_row(acc)


def last_kernel(plan, max_ref, base_ref, pos_ref, first_ref, acc_ref, step_ref,
                pos_out, vel_out, acc_out, steps_out, work_ref):
    rows, size = plan.rows, plan.size
    second = time_step_of(jnp.max(max_ref[...], axis=(0, 1), keepdims=True))
    one = step_ref[...]
    steps_out[0] = one[0, 0]
    steps_out[1] = second[0, 0]
    first = jnp.broadcast_to(one[:, :1], (rows, size))
    wide = jnp.broadcast_to(second, (rows, size))
    act = base_ref[7]
    for c in range(3):
        velocity = base_ref[4 + c] + first_ref[c] * first + acc_ref[c] * wide
        work_ref[0, c] = pos_ref[c] + velocity * act * wide
        work_ref[1, c] = velocity
    for t in range(plan.tiles):
        lanes = pl.ds(t * size, size)
        for c in range(3):
            pos_out[pl.ds(c, 1), lanes] = work_ref[0, c, pl.ds(t, 1), :]
            vel_out[pl.ds(c, 1), lanes] = work_ref[1, c, pl.ds(t, 1), :]
            acc_out[pl.ds(c, 1), lanes] = acc_ref[c, pl.ds(t, 1), :]


def vmem():
    return pl.BlockSpec(memory_space=pltpu.VMEM)


def hbm():
    return pl.BlockSpec(memory_space=pltpu.HBM)


def in_hbm(values):
    return pltpu.with_memory_space_constraint(values, pltpu.HBM)


def smem():
    return pl.BlockSpec(memory_space=pltpu.SMEM)


def call(kernel, outs, scratch, specs, name, out_specs=None):
    return pl.pallas_call(
        kernel,
        out_shape=outs,
        in_specs=specs,
        out_specs=out_specs or [vmem() for _ in outs],
        scratch_shapes=scratch,
        compiler_params=pltpu.CompilerParams(vmem_limit_bytes=VMEM_BYTES),
        name=name,
    )


def buffers(*shapes):
    return [pltpu.VMEM(shape, F32) for shape in shapes]


def floats(*shapes):
    return [jax.ShapeDtypeStruct(shape, F32) for shape in shapes]


def exchange(plan, block, bits):
    flip = sum(1 << bit for bit in bits)
    return lax.ppermute(block, AXES, [(i, i ^ flip) for i in range(plan.devices)])


def body(mesh, offsets, velocities, masses, active, near_local, near_remote, far_list):
    tiles, kl = near_local.shape
    kn = near_remote.shape[2]
    levels, km = far_list.shape[1:]
    size = masses.shape[0] // tiles
    plan = Plan(mesh, tiles, size, levels, km, kl, kn)
    rows, near_rows = plan.rows, plan.near_rows
    whole = (3, rows, size)
    extra = levels - 3
    base, moments, far_ids, *near = call(
        functools.partial(first_kernel, plan),
        floats((8, rows, size), (rows, size))
        + [jax.ShapeDtypeStruct((rows, size), jnp.int32)]
        + floats(*[(near_rows, size)] * 3),
        buffers(offsets.shape, velocities.shape, (tiles, size))
        + [
            pltpu.VMEM((tiles, size), jnp.int32),
            pltpu.VMEM((levels, km, tiles), jnp.int32),
            pltpu.SemaphoreType.DMA((5,)),
        ],
        [hbm()] * 5,
        "first",
    )(
        in_hbm(offsets),
        in_hbm(velocities),
        in_hbm(masses.reshape(tiles, size)),
        in_hbm(active.reshape(tiles, size)),
        in_hbm(jnp.transpose(far_list, (1, 2, 0))),
    )

    got_near = [None] * 3
    got_far = []
    for slot in range(3):
        got_near[slot] = exchange(plan, near[slot], [plan.near_level[slot]])
    for level in range(levels):
        if plan.place[level][2] < 0:
            got_far.append(exchange(plan, moments, [level]))

    lists = (
        in_hbm(jnp.transpose(near_local)),
        in_hbm(jnp.transpose(near_remote, (1, 2, 0))),
    )
    slots = (tiles, FAST_GROUPS * 8, size)
    broad = (tiles, 3, FAST_GROUPS * 8, size)
    list_scratch = [
        pltpu.SMEM((kl, tiles), jnp.int32),
        pltpu.SMEM((3, kn, tiles), jnp.int32),
        pltpu.SMEM((8, size), jnp.int32),
        pltpu.SemaphoreType.DMA((3,)),
    ]
    force_scratch = buffers((3, 4, up8(plan.face), size), broad, whole)
    rank, picks, order, comp, spread, local = call(
        functools.partial(local_kernel, plan),
        floats((rows, size))
        + [jax.ShapeDtypeStruct((levels * km, rows, size), BF16)]
        + [jax.ShapeDtypeStruct((8, size), jnp.int32)]
        + floats(slots, broad, broad),
        list_scratch[:2] + list_scratch[3:],
        [hbm(), hbm(), vmem(), vmem()],
        "local",
    )(*lists, base, far_ids)
    acc, packed, *send = call(
        functools.partial(second_kernel, plan),
        floats(whole, (8, size), *[(plan.frows, size)] * 3),
        force_scratch + list_scratch,
        [hbm(), hbm()] + [vmem()] * (6 + levels),
        "second",
    )(*lists, order, base, picks, rank, spread, local, *got_near, *got_far)
    slot_u, slot_a = call(
        functools.partial(gather_kernel, plan),
        floats(slots, slots),
        [],
        [vmem()] * 3,
        "gather",
    )(rank, comp, acc)

    got_send = [exchange(plan, send[slot], [plan.near_level[slot]]) for slot in range(3)]
    everyone = lax.all_to_all(
        jnp.broadcast_to(packed[None], (plan.devices, 8, size)), AXES, 0, 0
    )
    moved, acc2, square2, step = call(
        functools.partial(third_kernel, plan),
        floats(whole, whole, (1, size), (1, size)),
        force_scratch
        + buffers((4, rows, size), (3, plan.frows, size), slots, broad)
        + list_scratch,
        [hbm(), hbm()] + [vmem()] * (9 + 3 + 3 + extra),
        "third",
    )(
        *lists, order, base, picks, rank, comp, slot_u, slot_a, acc, everyone, *got_near, *got_send, *got_far,
    )
    copies = jnp.broadcast_to(square2[None], (plan.devices, 1, size))
    largest = lax.all_to_all(copies, AXES, 0, 0).reshape(plan.devices, size)
    pos, vel, out, steps = call(
        functools.partial(last_kernel, plan),
        floats(offsets.shape, offsets.shape, offsets.shape, (SUBSTEPS,)),
        buffers((2, 3, rows, size)),
        [vmem()] * 6,
        "last",
        [vmem(), vmem(), vmem(), smem()],
    )(largest, base, moved, acc, acc2, step)
    return pos, vel, out, steps


def solution(mesh):
    parts = P(None, AXES)
    return jax.shard_map(
        functools.partial(body, mesh),
        mesh=mesh,
        in_specs=(parts, parts, P(AXES), P(AXES), P(AXES, None), P(AXES, None, None), P(AXES, None, None)),
        out_specs=(parts, parts, parts, P()),
        check_vma=False,
    )
```
